128 devices in a mesh: section: 8 (over z, core), rows: 16 (over y, x).
Axes of the slice: x: 4, y: 4, z: 4, core: 2. Of those that a mesh axis runs over, the one named last changes fastest.
Arguments:
- features: bfloat16 [2048, 1536], P('rows'), may hold values from -6 to 6
- ages: int32 [2048], P('rows'), may hold values from 0 to 15
- age_table: bfloat16 [16, 1536], replicated, may hold values from -3 to 3
- returns: float32 [2048], P('rows'), may hold values from -6 to 6
- owners: int32 [2048, 1], P('rows'), may hold values from 0 to 15; in each aligned block of 128 rows (0 to 127, 128 to 255, ...) at most 32 rows name the same one
- slots: int32 [2048], P('rows'), may hold values from 0 to 4095
- norm_gain: float32 [8, 1536], P('section'), may hold values from 0.1 to 1.9
- w_gate: bfloat16 [8, 1536, 8960], P('section', None, 'rows'), may hold values from -0.15625 to 0.15625
- w_up: bfloat16 [8, 1536, 8960], P('section', None, 'rows'), may hold values from -0.15625 to 0.15625
- w_down: bfloat16 [8, 8960, 1536], P('section', 'rows'), may hold values from -0.0625 to 0.0625
- final_gain: float32 [1536], replicated, may hold values from 0.1 to 1.9
- reward_head: float32 [1536], replicated, may hold values from -0.15625 to 0.15625
- old_priority: float32 [65536], P('rows'), may hold values from 0.05 to 2
Outputs:
- rewards: float32 [2048], P(('rows', 'section'))
- weights: float32 [65536], P(('rows', 'section'))
The draws below stay inside these ranges and needn't reach their ends.
Inputs may be any that keep to these rules, and one draw needn't show every extreme that they name: `owners`: among the rows of one device at most 32 name the same owner; in every draw some owner is named by exactly 32 rows of some device.
All inputs are finite; a program needn't handle non-finite values.
Results may differ from the reference program's by a relative error of at most 0.04.
Values may be sent and summed in bfloat16 or wider, within the bound.
A program may use at most 64 MiB of HBM per device.

```python
import math
import jax
import jax.numpy as jnp
import numpy as np
from jax import lax

D = 1536
FF = 8960
AGES = 16
CAP = 32
ROWS_DEV = 128
BUF_DEV = 4096
LAYERS = 8
ROWS = 2048
OWNERS = 16
BUF = 65536


def set_ends(result, own_key, low, high):
    longest = result.shape.index(max(result.shape))
    spots = []
    for shift in (0, 1):
        where = [jax.random.randint(jax.random.fold_in(own_key, axis), (), 0, length) for axis, length in enumerate(result.shape)]
        where[longest] = (where[longest] + shift) % result.shape[longest]
        spots.append(tuple(where))
    return result.at[spots[0]].set(low).at[spots[1]].set(high)


def shard_levels(key, extent, cuts, least, high):
    loudness, own = 1.0, jax.random.fold_in(key, 6)
    for axis_at, parts in cuts:
        steps = jnp.exp(jax.random.uniform(jax.random.fold_in(own, axis_at), (parts,), jnp.float32, least / len(cuts), high / len(cuts)))
        loudness = loudness * jnp.repeat(steps, extent[axis_at] // parts).reshape([-1 if axis == axis_at else 1 for axis in range(len(extent))])
    return loudness


def assign_block(stream_key, own, number, rows, amount, top, reach, slope):
    order = jax.random.permutation(stream_key, amount)
    packed, usual = portions_of(amount, rows * top, reach, slope, True), portions_of(amount, rows * top, reach, slope, False)
    places = jnp.arange(amount)

    def named(lengths, rotation):
        used = int((lengths > 0).sum())
        fixed = max(1, used // 4)
        passed = fixed + (places - fixed + rotation * (used - fixed)) % max(1, amount - fixed)
        return jnp.zeros((amount,), jnp.int32).at[order[jnp.where(places < fixed, places, passed)]].set(jnp.asarray(lengths, jnp.int32))

    lengths = jnp.where(number % 4 == 0, named(packed, number // 4), named(usual, number - number // 4 - 1))
    mixed = jax.random.permutation(jax.random.fold_in(own, 3), amount)
    giver, sink = mixed[0:amount // 2 * 2:2], mixed[1:amount // 2 * 2:2]
    margin = jnp.minimum(lengths[giver] - 1, reach - lengths[sink]) // 2
    margin = jnp.where((giver == order[0]) | (sink == order[0]) | (lengths[sink] == 0), 0, jnp.maximum(margin, 0))
    passed = jax.random.randint(jax.random.fold_in(own, 4), (amount // 2,), 0, 1 << 20) % (margin + 1)
    lengths = lengths.at[giver].add(-passed).at[sink].add(passed)
    items = jnp.searchsorted(jnp.cumsum(lengths), jnp.arange(rows * top), side="right").astype(jnp.int32)
    grid = items.reshape(top, rows).T
    grid = grid[jax.random.permutation(jax.random.fold_in(own, 1), rows)]
    rotation = jax.random.randint(jax.random.fold_in(own, 2), (rows, 1), 0, top)
    return jnp.take_along_axis(grid, (jnp.arange(top)[None, :] + rotation) % top, axis=1)


def portions_of(count, total, reach, skew, full):
    loads = [(1 << 20) // math.isqrt(grade ** skew) + 1 for grade in range(1, count + 1)]
    largest = reach if full else min(reach, max(-(-total // count), total * loads[0] // sum(loads)))
    least = 1 if total - largest >= count - 1 else 0
    counts, surplus = [largest] + [least] * (count - 1), total - largest - least * (count - 1)
    while surplus > 0:
        candidates = [i for i in range(1, count) if counts[i] < largest] or [i for i in range(1, count) if counts[i] < reach]
        whole, budget = sum([loads[i] for i in candidates]), surplus
        for i in candidates:
            more = min(reach - counts[i], max(1, budget * loads[i] // whole), surplus)
            counts[i] = counts[i] + more
            surplus = surplus - more
    return np.array(counts)


def normal_values(key, dims, scale, most, split=(), dtype=jnp.bfloat16):
    result = scale * jax.random.normal(key, dims, jnp.float32)
    if split:
        result = result * shard_levels(key, dims, split, -0.22, 0.18)
    return jnp.clip(result, -most, most).astype(dtype)


def setup_inputs(seed: int = 0) -> dict:
    arg_keys = jax.random.split(jax.random.key(seed), 14)
    features = normal_values(arg_keys[0], (ROWS, D), 1.0, 6.0, ((0, 16),))
    ages = set_ends(jax.random.randint(arg_keys[1], (ROWS,), 0, AGES), jax.random.fold_in(arg_keys[1], 1), 0, AGES - 1).astype(jnp.int32)
    age_table = normal_values(arg_keys[2], (AGES, D), 0.5, 3.0)
    returns = normal_values(arg_keys[3], (ROWS,), 1.0, 6.0, ((0, 16),), jnp.float32)
    owners_keys = jax.random.split(jax.random.fold_in(arg_keys[4], 1), ROWS // ROWS_DEV)
    owners_turns = jax.random.permutation(jax.random.fold_in(arg_keys[4], 3), ROWS // ROWS_DEV)
    owners = jax.vmap(lambda own, number: assign_block(jax.random.fold_in(arg_keys[4], 2), own, number, ROWS_DEV, OWNERS, 1, CAP, 2))(owners_keys, owners_turns).reshape((ROWS, 1))
    slots = set_ends(jax.random.randint(arg_keys[5], (ROWS,), 0, BUF_DEV), jax.random.fold_in(arg_keys[5], 1), 0, BUF_DEV - 1).astype(jnp.int32)
    norm_gain = jnp.clip(1.0 + 0.18 * jax.random.normal(arg_keys[6], (LAYERS, D), jnp.float32), 0.1, 1.9)
    w_gate = normal_values(arg_keys[7], (LAYERS, D, FF), D ** -0.5, 0.15625, ((0, 8), (2, 16)))
    w_up = normal_values(arg_keys[8], (LAYERS, D, FF), D ** -0.5, 0.15625, ((0, 8), (2, 16)))
    w_down = normal_values(arg_keys[9], (LAYERS, FF, D), FF ** -0.5, 0.0625, ((0, 8), (1, 16)))
    final_gain = jnp.clip(1.0 + 0.18 * jax.random.normal(arg_keys[10], (D,), jnp.float32), 0.1, 1.9)
    reward_head = normal_values(arg_keys[11], (D,), D ** -0.5, 0.15625, (), jnp.float32)
    old_priority = jnp.clip(jnp.exp(math.log(2.0) - 3.6888794 * jax.random.uniform(arg_keys[12], (BUF,), jnp.float32) ** shard_levels(arg_keys[12], (BUF,), ((0, 16),), -0.2, 0.2)), 0.05, 2.0)
    return dict(features=features, ages=ages, age_table=age_table, returns=returns, owners=owners, slots=slots, norm_gain=norm_gain, w_gate=w_gate, w_up=w_up, w_down=w_down, final_gain=final_gain, reward_head=reward_head, old_priority=old_priority)


def scaled_norm(values, gain):
    return values * lax.rsqrt(lax.optimization_barrier(jnp.mean(values * values, axis=-1, keepdims=True)) + 1e-06) * gain

def reference(features, ages, age_table, returns, owners, slots, norm_gain, w_gate, w_up, w_down, final_gain, reward_head, old_priority):
    onehot = (ages[:, None] == jnp.arange(AGES)[None, :]).astype(jnp.bfloat16)
    state = (features.astype(jnp.float32) + jnp.dot(onehot, age_table, preferred_element_type=jnp.float32)).astype(jnp.bfloat16)
    for layer in range(LAYERS):
        wide = state.astype(jnp.float32)
        normed = scaled_norm(wide, norm_gain[layer]).astype(jnp.bfloat16)
        gate = jnp.dot(normed, w_gate[layer], preferred_element_type=jnp.float32)
        upper = jnp.dot(normed, w_up[layer], preferred_element_type=jnp.float32)
        hidden = (jax.nn.silu(gate) * upper).astype(jnp.bfloat16)
        state = (wide + jnp.dot(hidden, w_down[layer], preferred_element_type=jnp.float32)).astype(jnp.bfloat16)
    finished = scaled_norm(state.astype(jnp.float32), final_gain)
    rewards = lax.optimization_barrier(jnp.sum(finished * reward_head, axis=-1))
    priority = jnp.exp(0.6 * jnp.log(jnp.abs(rewards - returns) + 0.05))
    target = (owners[:, 0] * BUF_DEV + slots).astype(jnp.int32)
    largest = jax.ops.segment_max(priority, target, num_segments=BUF)
    counted = jax.ops.segment_sum(jnp.ones_like(priority), target, num_segments=BUF)
    refreshed = jnp.where(counted > 0, largest, old_priority)
    weights = refreshed * (BUF / jnp.sum(refreshed))
    return (rewards, weights)
```

```python
import functools

import jax
import jax.numpy as jnp
from jax import lax
from jax.experimental import pallas as pl
from jax.experimental.pallas import tpu as pltpu
from jax.sharding import PartitionSpec as P

MICRO = 16
SIDE = 4
MESH = pl.DeviceIdType.MESH
LANES = 128


def chunks(total, size):
    return [(at, min(size, total - at)) for at in range(0, total, size)]


def remote(src, dst, send_sem, recv_sem, where):
    return pltpu.make_async_remote_copy(
        src_ref=src, dst_ref=dst, send_sem=send_sem, recv_sem=recv_sem,
        device_id=where, device_id_type=MESH,
    )


def kernel(
    sections, groups,
    features, ages, age_table, returns, owners, slots, gain, w_gate, w_up, w_down,
    final_gain, head, old,
    rewards_out, weights_out,
    wg, wu, wd, w_both, state, gathered, hidden, part, part_in, line_out, line_in, last_in,
    final_row, reward_cols, marks, marks_wide, result, prio_wide, refreshed, sums,
    w_sem,
    in_send, ag_send, ag_recv, rs_send, rs_recv, ln_send, ln_recv, fn_recv,
    mk_send, mk_recv, up_send, up_recv, rw_send, rw_recv, sm_send, sm_recv,
):
    sec = lax.axis_index("section")
    me = lax.axis_index("rows")
    spot = (lax.rem(me, SIDE), me // SIDE)
    block, width = state.shape[2], state.shape[3]
    rows = features.shape[0]
    ff = hidden.shape[1]
    even = ff // 256 * 256
    rest = ff - even
    last = sections - 1
    rounds = MICRO // SIDE

    def step_on(axis, d):
        return lax.rem(spot[axis] + d, SIDE)

    def on_line(axis, index):
        return spot[1] * SIDE + index if axis == 0 else index * SIDE + spot[0]

    loads = [
        pltpu.make_async_copy(w_gate, wg, w_sem.at[0]),
        pltpu.make_async_copy(w_up, wu, w_sem.at[1]),
        pltpu.make_async_copy(w_down, wd, w_sem.at[2]),
    ]
    for load in loads:
        load.start()

    barrier = pltpu.get_barrier_semaphore()
    for j in range(1, groups):
        pl.semaphore_signal(barrier, inc=1, device_id={"rows": lax.rem(me + j, groups)}, device_id_type=MESH)
    for j in range(1, sections):
        pl.semaphore_signal(barrier, inc=1, device_id={"section": lax.rem(sec + j, sections)}, device_id_type=MESH)
    before = lax.rem(sec + last, sections)
    for axis in range(2):
        for d in range(1, SIDE):
            pl.semaphore_signal(
                barrier, inc=1, device_id={"section": before, "rows": on_line(axis, step_on(axis, d))}, device_id_type=MESH
            )

    marks[me] = (owners[...] * (old.shape[0] * LANES) + slots[...]).astype(jnp.float32)

    for i in range(final_gain.shape[0]):
        final_row[0:1, i * LANES:(i + 1) * LANES] = final_gain[i:i + 1, :]
        final_row[1:2, i * LANES:(i + 1) * LANES] = head[i:i + 1, :]

    @pl.when(sec == 0)
    def _():
        tall = jnp.transpose(jnp.broadcast_to(ages[...].astype(jnp.float32), (LANES, rows)))
        buckets = age_table.shape[0]
        onehot = (
            tall[:, :buckets] == lax.broadcasted_iota(jnp.int32, (rows, buckets), 1).astype(jnp.float32)
        ).astype(jnp.float32).astype(jnp.bfloat16)
        for at, size in chunks(width, 512):
            entry = features[:, at:at + size].astype(jnp.float32) + jnp.dot(
                onehot, age_table[:, at:at + size], preferred_element_type=jnp.float32
            )
            entry = entry.astype(jnp.bfloat16).reshape(2, rounds, block, size)
            for h in range(2):
                for k in range(rounds):
                    state[k * SIDE + spot[1 - h], h, :, at:at + size] = entry[h, k]

    pl.semaphore_wait(barrier, groups - 1 + sections - 1 + 2 * (SIDE - 1))

    def to_group(ref, send, recv, j):
        return remote(ref.at[me], ref.at[me], send.at[j], recv.at[j], {"rows": lax.rem(me + j, groups)})

    def from_group(ref, send, recv, j):
        spot_ref = ref.at[lax.rem(me + groups - j, groups)]
        return remote(spot_ref, spot_ref, send.at[j], recv.at[j], {"rows": lax.rem(me + j, groups)})

    def in_copy(k, h, d):
        t = k * SIDE + spot[1 - h]
        ref = state.at[t, h]
        return remote(
            ref, ref, in_send.at[k, h, d - 1], ln_recv.at[t, h, 0], {"rows": on_line(1 - h, step_on(1 - h, d))}
        )

    def in_from(t, h):
        ref = state.at[t, h]
        return remote(ref, ref, in_send.at[0, h, 0], ln_recv.at[t, h, 0], {"rows": on_line(1 - h, step_on(1 - h, 1))})

    def ag_copy(t, h, d, shard):
        ref = gathered.at[t, h, shard]
        return remote(
            ref, ref, ag_send.at[t, h, d - 1], ag_recv.at[t, h, d - 1], {"rows": on_line(h, step_on(h, d))}
        )

    def rs_copy(t, h, d):
        return remote(
            part.at[t, h, step_on(h, d)], part_in.at[t, h, d - 1], rs_send.at[t, h, d - 1], rs_recv.at[t, h, d - 1],
            {"rows": on_line(h, step_on(h, d))},
        )

    def line_copy(t, h, d):
        own = spot[1 - h]
        return remote(
            line_out.at[t, h], line_in.at[t, h, own], ln_send.at[t, h, d], ln_recv.at[t, h, own],
            {"section": jnp.minimum(sec + 1, last), "rows": on_line(1 - h, step_on(1 - h, d))},
        )

    def line_from(t, h, i):
        return remote(
            line_out.at[t, h], line_in.at[t, h, i], ln_send.at[t, h, 0], ln_recv.at[t, h, i],
            {"section": jnp.maximum(sec - 1, 0)},
        )

    def home_of(t):
        return lax.rem(t, SIDE)

    def last_copy(t, h):
        home = home_of(t)
        d = lax.rem(home + SIDE - spot[1 - h] + SIDE - 1, SIDE)
        k = t // SIDE
        return remote(
            line_out.at[t, h], last_in.at[k, h, d], ln_send.at[t, h, 0], fn_recv.at[k, h, d],
            {"rows": on_line(1 - h, home)},
        )

    def last_from(k, h, d):
        ref = last_in.at[k, h, d - 1]
        return remote(ref, ref, ln_send.at[0, h, 0], fn_recv.at[k, h, d - 1], {"rows": on_line(1 - h, step_on(1 - h, d))})

    def enter(t):
        for h in range(2):
            @pl.when(sec > 0)
            def _():
                for i in range(SIDE):
                    line_from(t, h, i).wait_recv()
                total = line_in[t, h, 0].astype(jnp.float32)
                for i in range(1, SIDE):
                    total = total + line_in[t, h, i].astype(jnp.float32)
                state[t, h] = total.astype(jnp.bfloat16)

            @pl.when((sec == 0) & (spot[1 - h] != home_of(t)))
            def _():
                in_from(t, h).wait_recv()

            wide = state[t, h].astype(jnp.float32)
            scale = lax.rsqrt(jnp.mean(wide * wide, axis=-1, keepdims=True) + 1e-06)
            gathered[t, h, spot[h]] = (wide * scale * gain[...]).astype(jnp.bfloat16)
            for d in (2, 1, 3):
                ag_copy(t, h, d, spot[h]).start()

    def work(t):
        for h in range(2):
            for d in (1, 3, 2):
                ag_copy(t, h, d, step_on(h, SIDE - d)).wait_recv()
        piece = gathered[t].reshape(2 * SIDE * block, width)
        for at in range(0, even, 256):
            gate = jnp.dot(piece, w_both[:, at:at + 256], preferred_element_type=jnp.float32)
            upper = jnp.dot(piece, w_both[:, even + at:even + at + 256], preferred_element_type=jnp.float32)
            hidden[:, at:at + 256] = (gate / (1.0 + jnp.exp(-gate)) * upper).astype(jnp.bfloat16)
        ends = jnp.dot(piece, w_both[:, 2 * even:2 * even + 256], preferred_element_type=jnp.float32)
        gate, upper = ends[:, :rest], ends[:, LANES:LANES + rest]
        hidden[:, even:ff] = (gate / (1.0 + jnp.exp(-gate)) * upper).astype(jnp.bfloat16)
        units = hidden[...]
        for at, size in chunks(width, 256):
            down = jnp.dot(units, wd[:, at:at + size], preferred_element_type=jnp.float32)
            part[t, :, :, :, at:at + size] = down.astype(jnp.bfloat16).reshape(2, SIDE, block, size)
        for h in range(2):
            for d in (2, 1, 3):
                rs_copy(t, h, d).start()

    def leave(t):
        home = home_of(t)
        for h in range(2):
            total = part[t, h, spot[h]].astype(jnp.float32)
            total = total + jnp.where(spot[1 - h] == home, state[t, h].astype(jnp.float32), 0.0)
            for d in range(1, SIDE):
                rs_copy(t, h, d).wait_recv()
                total = total + part_in[t, h, d - 1].astype(jnp.float32)
            line_out[t, h] = total.astype(jnp.bfloat16)

            @pl.when(sec < last)
            def _():
                for d in (2, 1, 3, 0):
                    line_copy(t, h, d).start()

            @pl.when((sec == last) & (spot[1 - h] != home))
            def _():
                last_copy(t, h).start()

    def finish(t):
        k = t // SIDE
        for h in range(2):
            @pl.when(spot[1 - h] == home_of(t))
            def _():
                total = line_out[t, h].astype(jnp.float32)
                for d in range(1, SIDE):
                    last_from(k, h, d).wait_recv()
                    total = total + last_in[k, h, d - 1].astype(jnp.float32)
                wide = total.astype(jnp.bfloat16).astype(jnp.float32)
                scale = lax.rsqrt(jnp.mean(wide * wide, axis=-1, keepdims=True) + 1e-06)
                value = jnp.sum(wide * scale * final_row[0:1] * final_row[1:2], axis=-1, keepdims=True)
                reward_cols[h, k] = jnp.broadcast_to(value, (block, LANES))

    @pl.when(sec == 0)
    def _():
        for k in range(rounds):
            for h in range(2):
                for d in (2, 1, 3):
                    in_copy(k, h, d).start()

    def turned(load, flat, first):
        load.wait()
        for at in range(0, even, 256):
            w_both[:, first * even + at:first * even + at + 256] = jnp.transpose(flat[at:at + 256, :])
        w_both[:, 2 * even + first * LANES:2 * even + first * LANES + rest] = jnp.transpose(flat[even:ff, :])

    w_both[:, 2 * even:2 * even + 256] = jnp.zeros((width, 256), jnp.bfloat16)
    turned(loads[0], wg, 0)
    for j in range(1, groups):
        to_group(marks, mk_send, mk_recv, j).start()

    @pl.when(sec == 0)
    def _():
        enter(0)

    turned(loads[1], wu, 1)
    loads[2].wait()

    @pl.when(sec > 0)
    def _():
        enter(0)

    def step(t, carry):
        work(t)

        @pl.when(t + 1 < MICRO)
        def _():
            enter(t + 1)

        @pl.when((sec == last) & (t > 0))
        def _():
            finish(t - 1)

        leave(t)
        return carry

    lax.fori_loop(0, MICRO, step, 0)

    for j in range(1, groups):
        from_group(marks, mk_send, mk_recv, j).wait_recv()
    for r in range(groups):
        marks_wide[r] = jnp.transpose(jnp.broadcast_to(marks[r], (LANES, rows)))

    def up_copy(j):
        return remote(result.at[me], result.at[me], up_send.at[j - 1], up_recv.at[0], {"section": last - j})

    @pl.when(sec == last)
    def _():
        finish(MICRO - 1)
        square = reward_cols[...].reshape(rows, LANES)
        on_diagonal = lax.broadcasted_iota(jnp.int32, (rows, rows), 0) == lax.broadcasted_iota(jnp.int32, (rows, rows), 1)
        row = jnp.sum(jnp.where(on_diagonal, square, 0.0), axis=0, keepdims=True)
        priority = jnp.exp(0.6 * jnp.log(jnp.abs(row - returns[...]) + 0.05))
        result[me, 0:1] = row
        result[me, 1:2] = priority
        for j in range(1, sections):
            up_copy(j).start()

    @pl.when(sec < last)
    def _():
        up_copy(1).wait_recv()

    for j in range(1, groups):
        to_group(result, rw_send, rw_recv, j).start()

    mine = result[me, 0:1]
    share = rows // sections
    picked = mine[:, 0:share]
    for s in range(1, sections):
        picked = jnp.where(sec == s, mine[:, s * share:(s + 1) * share], picked)
    rewards_out[...] = picked

    for j in range(1, groups):
        from_group(result, rw_send, rw_recv, j).wait_recv()
    for r in range(groups):
        prio_wide[r] = jnp.transpose(jnp.broadcast_to(result[r, 1:2], (LANES, rows)))

    lines = old.shape[0]
    table = lines * LANES
    batch = 4
    lane = lax.broadcasted_iota(jnp.int32, (1, LANES), 1).astype(jnp.float32)

    def match(g, carry):
        first = (me * table + g * (batch * LANES)).astype(jnp.float32)
        names = [first + (q * LANES) + lane for q in range(batch)]

        def one(r, best):
            best = list(best)
            for i in range(0, rows, 8):
                mark = marks_wide[r, i:i + 8, :]
                prio = prio_wide[r, i:i + 8, :]
                for q in range(batch):
                    best[q] = jnp.maximum(best[q], jnp.where(mark == names[q], prio, 0.0))
            return tuple(best)

        best = lax.fori_loop(0, groups, one, tuple(jnp.zeros((8, LANES), jnp.float32) for _ in range(batch)))
        for q in range(batch):
            top = jnp.max(best[q], axis=0, keepdims=True)
            at = pl.ds(g * batch + q, 1)
            refreshed[at, :] = jnp.where(top > 0.0, top, old[at, :])
        return carry

    lax.fori_loop(0, lines // batch, match, 0)
    subtotal = jnp.sum(jnp.sum(refreshed[...], axis=0, keepdims=True), axis=1, keepdims=True)
    sums[me] = jnp.broadcast_to(subtotal, (1, LANES))
    for j in range(1, groups):
        to_group(sums, sm_send, sm_recv, j).start()

    def drain(t, carry):
        for h in range(2):
            for d in range(1, SIDE):
                ag_copy(t, h, d, spot[h]).wait_send()
                rs_copy(t, h, d).wait_send()

            @pl.when(sec < last)
            def _():
                for d in range(SIDE):
                    line_copy(t, h, d).wait_send()

            @pl.when((sec == last) & (spot[1 - h] != home_of(t)))
            def _():
                last_copy(t, h).wait_send()
        return carry

    lax.fori_loop(0, MICRO, drain, 0)

    @pl.when(sec == 0)
    def _():
        for k in range(rounds):
            for h in range(2):
                for d in range(1, SIDE):
                    in_copy(k, h, d).wait_send()

    @pl.when(sec == last)
    def _():
        for j in range(1, sections):
            up_copy(j).wait_send()

    for j in range(1, groups):
        to_group(marks, mk_send, mk_recv, j).wait_send()
        to_group(result, rw_send, rw_recv, j).wait_send()

    for j in range(1, groups):
        from_group(sums, sm_send, sm_recv, j).wait_recv()
    total = sums[0]
    for r in range(1, groups):
        total = total + sums[r]
    tall = lines // sections
    weights_out[...] = refreshed[pl.ds(sec * tall, tall), :] * (table * groups / total)
    for j in range(1, groups):
        to_group(sums, sm_send, sm_recv, j).wait_send()


def handed(rewards, weights, rewards_out, weights_out):
    rewards_out[...] = rewards[...]
    weights_out[...] = weights[...]


def on_device(
    features, ages, age_table, returns, owners, slots, norm_gain,
    w_gate, w_up, w_down, final_gain, reward_head, old_priority,
):
    sections, groups = lax.axis_size("section"), lax.axis_size("rows")
    rows, width = features.shape
    block = rows * groups // (MICRO * 2 * SIDE)
    rounds = MICRO // SIDE
    ff = w_gate.shape[2]
    even = ff // 256 * 256
    table = old_priority.shape[0]
    lines = table // LANES
    vmem = pl.BlockSpec(memory_space=pltpu.VMEM)
    far = pl.BlockSpec(memory_space=pl.ANY)
    bf16, f32, dma = jnp.bfloat16, jnp.float32, pltpu.SemaphoreType.DMA
    rewards, weights = pl.pallas_call(
        functools.partial(kernel, sections, groups),
        out_shape=(
            jax.ShapeDtypeStruct((1, rows // sections), f32),
            jax.ShapeDtypeStruct((lines // sections, LANES), f32),
        ),
        in_specs=[vmem] * 7 + [far] * 3 + [vmem] * 3,
        out_specs=(vmem, vmem),
        scratch_shapes=[
            pltpu.VMEM((ff, width), bf16),
            pltpu.VMEM((ff, width), bf16),
            pltpu.VMEM((ff, width), bf16),
            pltpu.VMEM((width, 2 * even + 256), bf16),
            pltpu.VMEM((MICRO, 2, block, width), bf16),
            pltpu.VMEM((MICRO, 2, SIDE, block, width), bf16),
            pltpu.VMEM((2 * SIDE * block, ff), bf16),
            pltpu.VMEM((MICRO, 2, SIDE, block, width), bf16),
            pltpu.VMEM((MICRO, 2, SIDE - 1, block, width), bf16),
            pltpu.VMEM((MICRO, 2, block, width), bf16),
            pltpu.VMEM((MICRO, 2, SIDE, block, width), bf16),
            pltpu.VMEM((rounds, 2, SIDE - 1, block, width), bf16),
            pltpu.VMEM((2, width), f32),
            pltpu.VMEM((2, rounds, block, LANES), f32),
            pltpu.VMEM((groups, 1, rows), f32),
            pltpu.VMEM((groups, rows, LANES), f32),
            pltpu.VMEM((groups, 2, rows), f32),
            pltpu.VMEM((groups, rows, LANES), f32),
            pltpu.VMEM((lines, LANES), f32),
            pltpu.VMEM((groups, 1, LANES), f32),
            dma((3,)),
            dma((rounds, 2, SIDE - 1)),
            dma((MICRO, 2, SIDE - 1)), dma((MICRO, 2, SIDE - 1)),
            dma((MICRO, 2, SIDE - 1)), dma((MICRO, 2, SIDE - 1)),
            dma((MICRO, 2, SIDE)), dma((MICRO, 2, SIDE)),
            dma((rounds, 2, SIDE - 1)),
            dma((groups,)), dma((groups,)),
            dma((sections - 1,)), dma((1,)),
            dma((groups,)), dma((groups,)),
            dma((groups,)), dma((groups,)),
        ],
        compiler_params=pltpu.CompilerParams(
            collective_id=0, has_side_effects=True, vmem_limit_bytes=56 * 1024 * 1024
        ),
        name="refresh",
    )(
        features, ages.reshape(1, rows), age_table, returns.reshape(1, rows),
        owners.reshape(1, rows), slots.reshape(1, rows),
        norm_gain, w_gate[0].T, w_up[0].T, w_down[0],
        final_gain.reshape(-1, LANES), reward_head.reshape(-1, LANES),
        old_priority.reshape(lines, LANES),
    )
    rewards, weights = pl.pallas_call(
        handed, out_shape=tuple(jax.ShapeDtypeStruct(each.shape, f32) for each in (rewards, weights)),
        in_specs=[vmem, vmem], out_specs=(vmem, vmem), name="handed",
    )(rewards, weights)
    return rewards.reshape(-1), weights.reshape(-1)


def solution(mesh):
    placed = (
        P("rows", None),
        P("rows"),
        P(),
        P("rows"),
        P("rows", None),
        P("rows"),
        P("section", None),
        P("section", None, "rows"),
        P("section", None, "rows"),
        P("section", "rows", None),
        P(),
        P(),
        P("rows"),
    )
    return jax.shard_map(
        on_device,
        mesh=mesh,
        in_specs=placed,
        out_specs=(P(("rows", "section")), P(("rows", "section"))),
        check_vma=False,
    )
```

```python
import functools

import jax
import jax.numpy as jnp
from jax import lax
from jax.experimental import pallas as pl
from jax.experimental.pallas import tpu as pltpu
from jax.sharding import PartitionSpec as P

MICRO = 32
ENTER_AHEAD = 3
WORK_AHEAD = 2
RING = 8
SIDE = 4
MESH = pl.DeviceIdType.MESH
LANES = 128


def chunks(total, size):
    return [(at, min(size, total - at)) for at in range(0, total, size)]


def remote(src, dst, send_sem, recv_sem, where):
    return pltpu.make_async_remote_copy(
        src_ref=src, dst_ref=dst, send_sem=send_sem, recv_sem=recv_sem,
        device_id=where, device_id_type=MESH,
    )


def kernel(
    sections, groups,
    features, ages, age_table, returns, owners, slots, gain, w_gate, w_up, w_down,
    final_gain, head, old,
    rewards_out, weights_out,
    wg, wu, wd, w_both, state, gathered, hidden, part, part_in, line_out, line_in, last_in,
    final_row, reward_cols, marks, marks_wide, result, prio_wide, tops, shares, spare, sums,
    w_sem,
    in_send, ag_send, ag_recv, rs_send, rs_recv, ln_send, ln_recv, fn_recv,
    mk_send, mk_recv, up_send, up_recv, rw_send, rw_recv, sm_send, sm_recv,
):
    sec = lax.axis_index("section")
    me = lax.axis_index("rows")
    spot = (lax.rem(me, SIDE), me // SIDE)
    block, width = state.shape[2], state.shape[3]
    rows = features.shape[0]
    ff = hidden.shape[1]
    even = ff // 256 * 256
    rest = ff - even
    last = sections - 1
    rounds = MICRO // SIDE

    def step_on(axis, d):
        return lax.rem(spot[axis] + d, SIDE)

    def on_line(axis, index):
        return spot[1] * SIDE + index if axis == 0 else index * SIDE + spot[0]

    loads = [
        pltpu.make_async_copy(w_gate, wg, w_sem.at[0]),
        pltpu.make_async_copy(w_up, wu, w_sem.at[1]),
        pltpu.make_async_copy(w_down, wd, w_sem.at[2]),
    ]
    for load in loads:
        load.start()

    barrier = pltpu.get_barrier_semaphore()
    for j in range(1, groups):
        pl.semaphore_signal(barrier, inc=1, device_id={"rows": lax.rem(me + j, groups)}, device_id_type=MESH)
    for j in range(1, sections):
        pl.semaphore_signal(barrier, inc=1, device_id={"section": lax.rem(sec + j, sections)}, device_id_type=MESH)
    before = lax.rem(sec + last, sections)
    for axis in range(2):
        for d in range(1, SIDE):
            pl.semaphore_signal(
                barrier, inc=1, device_id={"section": before, "rows": on_line(axis, step_on(axis, d))}, device_id_type=MESH
            )

    marks[me] = (owners[...] * (old.shape[0] * LANES) + slots[...]).astype(jnp.float32)

    for i in range(final_gain.shape[0]):
        final_row[0:1, i * LANES:(i + 1) * LANES] = final_gain[i:i + 1, :]
        final_row[1:2, i * LANES:(i + 1) * LANES] = head[i:i + 1, :]

    @pl.when(sec == 0)
    def _():
        tall = jnp.transpose(jnp.broadcast_to(ages[...].astype(jnp.float32), (LANES, rows)))
        buckets = age_table.shape[0]
        onehot = (
            tall[:, :buckets] == lax.broadcasted_iota(jnp.int32, (rows, buckets), 1).astype(jnp.float32)
        ).astype(jnp.float32).astype(jnp.bfloat16)
        for at, size in chunks(width, 512):
            entry = features[:, at:at + size].astype(jnp.float32) + jnp.dot(
                onehot, age_table[:, at:at + size], preferred_element_type=jnp.float32
            )
            entry = entry.astype(jnp.bfloat16).reshape(2, rounds, block, size)
            for h in range(2):
                for k in range(rounds):
                    state[k * SIDE + spot[1 - h], h, :, at:at + size] = entry[h, k]

    def turned(load, flat, first):
        load.wait()
        for at in range(0, even, 256):
            w_both[:, first * even + at:first * even + at + 256] = jnp.transpose(flat[at:at + 256, :])
        w_both[:, 2 * even + first * LANES:2 * even + first * LANES + rest] = jnp.transpose(flat[even:ff, :])

    w_both[:, 2 * even:2 * even + 256] = jnp.zeros((width, 256), jnp.bfloat16)
    turned(loads[0], wg, 0)
    turned(loads[1], wu, 1)
    loads[2].wait()

    pl.semaphore_wait(barrier, groups - 1 + sections - 1 + 2 * (SIDE - 1))

    here = {"rows": lax.rem(me + 1, groups)}

    def arrived(ref, recv):
        remote(ref, ref, in_send.at[0], recv, here).wait_recv()

    def departed(ref, send):
        remote(ref, ref, send, ln_recv.at[0, 0], here).wait_send()

    def to_group(ref, send, recv, j):
        return remote(ref.at[me], ref.at[me], send.at[0], recv.at[0], {"rows": lax.rem(me + j, groups)})

    def all_but_one(ref):
        return ref.at[pl.ds(0, groups - 1)]

    def in_copy(k, h, d):
        t = k * SIDE + spot[1 - h]
        ref = state.at[t, h]
        return remote(ref, ref, in_send.at[0], ln_recv.at[t, h], {"rows": on_line(1 - h, step_on(1 - h, d))})

    def ag_copy(t, h, d):
        ref = gathered.at[t, h, spot[h]]
        return remote(ref, ref, ag_send.at[0], ag_recv.at[lax.rem(t, RING), h], {"rows": on_line(h, step_on(h, d))})

    def rs_copy(t, h, d):
        return remote(
            part.at[t, h, step_on(h, d)], part_in.at[t, h, d - 1], rs_send.at[0], rs_recv.at[lax.rem(t, RING), h],
            {"rows": on_line(h, step_on(h, d))},
        )

    def line_copy(t, h, d):
        return remote(
            line_out.at[t, h], line_in.at[t, h, spot[1 - h]], ln_send.at[0], ln_recv.at[t, h],
            {"section": jnp.minimum(sec + 1, last), "rows": on_line(1 - h, step_on(1 - h, d))},
        )

    def home_of(t):
        return lax.rem(t, SIDE)

    def last_copy(t, h):
        home = home_of(t)
        d = lax.rem(home + SIDE - spot[1 - h] + SIDE - 1, SIDE)
        k = t // SIDE
        return remote(
            line_out.at[t, h], last_in.at[k, h, d], ln_send.at[0], fn_recv.at[k, h],
            {"rows": on_line(1 - h, home)},
        )

    def enter(t):
        for h in range(2):
            @pl.when(sec > 0)
            def _():
                arrived(line_in.at[t, h], ln_recv.at[t, h])
                total = line_in[t, h, 0].astype(jnp.float32)
                for i in range(1, SIDE):
                    total = total + line_in[t, h, i].astype(jnp.float32)
                state[t, h] = total.astype(jnp.bfloat16)

            @pl.when((sec == 0) & (spot[1 - h] != home_of(t)))
            def _():
                arrived(state.at[t, h], ln_recv.at[t, h])

            wide = state[t, h].astype(jnp.float32)
            scale = lax.rsqrt(jnp.mean(wide * wide, axis=-1, keepdims=True) + 1e-06)
            gathered[t, h, spot[h]] = (wide * scale * gain[...]).astype(jnp.bfloat16)
            for d in (2, 1, 3):
                ag_copy(t, h, d).start()

    def work(t):
        for h in range(2):
            arrived(gathered.at[t, h, pl.ds(0, SIDE - 1)], ag_recv.at[lax.rem(t, RING), h])
        piece = gathered[t].reshape(2 * SIDE * block, width)
        for at in range(0, even, 256):
            gate = jnp.dot(piece, w_both[:, at:at + 256], preferred_element_type=jnp.float32)
            upper = jnp.dot(piece, w_both[:, even + at:even + at + 256], preferred_element_type=jnp.float32)
            hidden[:, at:at + 256] = (gate / (1.0 + jnp.exp(-gate)) * upper).astype(jnp.bfloat16)
        ends = jnp.dot(piece, w_both[:, 2 * even:2 * even + 256], preferred_element_type=jnp.float32)
        gate, upper = ends[:, :rest], ends[:, LANES:LANES + rest]
        hidden[:, even:ff] = (gate / (1.0 + jnp.exp(-gate)) * upper).astype(jnp.bfloat16)
        units = hidden[...]
        for at, size in chunks(width, 256):
            down = jnp.dot(units, wd[:, at:at + size], preferred_element_type=jnp.float32)
            part[t, :, :, :, at:at + size] = down.astype(jnp.bfloat16).reshape(2, SIDE, block, size)
        for h in range(2):
            for d in (2, 1, 3):
                rs_copy(t, h, d).start()

    def leave(t):
        home = home_of(t)
        for h in range(2):
            total = part[t, h, spot[h]].astype(jnp.float32)
            total = total + jnp.where(spot[1 - h] == home, state[t, h].astype(jnp.float32), 0.0)
            arrived(part_in.at[t, h], rs_recv.at[lax.rem(t, RING), h])
            for d in range(1, SIDE):
                total = total + part_in[t, h, d - 1].astype(jnp.float32)
            line_out[t, h] = total.astype(jnp.bfloat16)

            @pl.when(sec < last)
            def _():
                for d in (2, 1, 3, 0):
                    line_copy(t, h, d).start()

            @pl.when((sec == last) & (spot[1 - h] != home))
            def _():
                last_copy(t, h).start()

    def finish(t):
        k = t // SIDE
        for h in range(2):
            @pl.when(spot[1 - h] == home_of(t))
            def _():
                total = line_out[t, h].astype(jnp.float32)
                arrived(last_in.at[k, h], fn_recv.at[k, h])
                for d in range(1, SIDE):
                    total = total + last_in[k, h, d - 1].astype(jnp.float32)
                wide = total.astype(jnp.bfloat16).astype(jnp.float32)
                scale = lax.rsqrt(jnp.mean(wide * wide, axis=-1, keepdims=True) + 1e-06)
                value = jnp.sum(wide * scale * final_row[0:1] * final_row[1:2], axis=-1, keepdims=True)
                reward_cols[h, k] = jnp.broadcast_to(value, (block, LANES))

    @pl.when(sec == 0)
    def _():
        for k in range(rounds):
            for h in range(2):
                for d in (2, 1, 3):
                    in_copy(k, h, d).start()

    for j in range(1, groups):
        to_group(marks, mk_send, mk_recv, j).start()

    lines = old.shape[0]
    table = lines * LANES
    tall = lines // sections
    batch = 4
    lane = lax.broadcasted_iota(jnp.int32, (1, LANES), 1).astype(jnp.float32)

    def over_rows(names, join):
        def one(r, best):
            best = list(best)
            for i in range(0, rows, 8):
                mark = marks_wide[r, i:i + 8, :]
                value = prio_wide[r, i:i + 8, :]
                for q in range(batch):
                    best[q] = join(best[q], jnp.where(mark == names[q], value, 0.0))
            return tuple(best)

        return lax.fori_loop(0, groups, one, tuple(jnp.zeros((8, LANES), jnp.float32) for _ in range(batch)))

    def count():
        arrived(all_but_one(marks), mk_recv.at[0])
        for r in range(groups):
            marks_wide[r] = jnp.transpose(jnp.broadcast_to(marks[r], (LANES, rows)))
            prio_wide[r] = jnp.ones((rows, LANES), jnp.float32)

        def by_row(g, carry):
            found = over_rows([marks[g * batch + q] for q in range(batch)], jnp.add)
            for q in range(batch):
                shares[g * batch + q] = 1.0 / jnp.sum(found[q], axis=0, keepdims=True)
            return carry

        lax.fori_loop(0, groups // batch, by_row, 0)

        def by_entry(g, carry):
            first = (me * table + g * (batch * LANES)).astype(jnp.float32)
            found = over_rows([first + (q * LANES) + lane for q in range(batch)], jnp.add)
            for q in range(batch):
                at = pl.ds(g * batch + q, 1)
                spare[at, :] = jnp.where(jnp.sum(found[q], axis=0, keepdims=True) > 0.0, 0.0, old[at, :])
            return carry

        lax.fori_loop(0, lines // batch, by_entry, 0)
        subtotal = jnp.sum(jnp.sum(spare[...], axis=0, keepdims=True), axis=1, keepdims=True)
        sums[me] = jnp.broadcast_to(subtotal, (1, LANES))
        for j in range(1, groups):
            to_group(sums, sm_send, sm_recv, j).start()

    @pl.when(sec >= sections // 2)
    def _():
        count()

    def step(i, carry):
        t = i - ENTER_AHEAD

        @pl.when((sec == last) & (t >= 2))
        def _():
            finish(t - 2)

        @pl.when(t >= 0)
        def _():
            leave(t)

        @pl.when(i < MICRO)
        def _():
            enter(i)

        @pl.when((t + WORK_AHEAD >= 0) & (t + WORK_AHEAD < MICRO))
        def _():
            work(t + WORK_AHEAD)

        return carry

    lax.fori_loop(0, MICRO + ENTER_AHEAD, step, 0)

    @pl.when(sec < sections // 2)
    def _():
        count()

    def up_copy(j):
        return remote(result.at[me], result.at[me], up_send.at[0], up_recv.at[0], {"section": last - j})

    @pl.when(sec == last)
    def _():
        finish(MICRO - 2)
        finish(MICRO - 1)
        square = reward_cols[...].reshape(rows, LANES)
        on_diagonal = lax.broadcasted_iota(jnp.int32, (rows, rows), 0) == lax.broadcasted_iota(jnp.int32, (rows, rows), 1)
        row = jnp.sum(jnp.where(on_diagonal, square, 0.0), axis=0, keepdims=True)
        priority = jnp.exp(0.6 * jnp.log(jnp.abs(row - returns[...]) + 0.05))
        result[me, 0:1] = row
        result[me, 1:2] = priority
        for j in range(1, sections):
            up_copy(j).start()

    departed(part_in, ag_send.at[0])
    departed(part_in, rs_send.at[0])
    departed(all_but_one(marks), mk_send.at[0])

    @pl.when(sec == 0)
    def _():
        departed(part_in.at[pl.ds(0, rounds)], in_send.at[0])

    arrived(all_but_one(sums), sm_recv.at[0])
    departed(all_but_one(sums), sm_send.at[0])
    kept = sums[0]
    for r in range(1, groups):
        kept = kept + sums[r]

    @pl.when(sec < last)
    def _():
        departed(line_in, ln_send.at[0])
        arrived(result.at[me], up_recv.at[0])

    for j in range(1, groups):
        to_group(result, rw_send, rw_recv, j).start()

    @pl.when(sec == last)
    def _():
        departed(part_in.at[pl.ds(0, rounds)], ln_send.at[0])

    mine = result[me, 0:1]
    share = rows // sections
    picked = mine[:, 0:share]
    for s in range(1, sections):
        picked = jnp.where(sec == s, mine[:, s * share:(s + 1) * share], picked)
    rewards_out[...] = picked

    arrived(all_but_one(result), rw_recv.at[0])
    for r in range(groups):
        prio_wide[r] = jnp.transpose(jnp.broadcast_to(result[r, 1:2], (LANES, rows)))

    def by_row(g, carry):
        found = over_rows([marks[g * batch + q] for q in range(batch)], jnp.maximum)
        for q in range(batch):
            tops[g * batch + q] = jnp.max(found[q], axis=0, keepdims=True) * shares[g * batch + q]
        return carry

    lax.fori_loop(0, groups // batch, by_row, 0)
    named = jnp.sum(jnp.sum(tops[...], axis=0), axis=1, keepdims=True)
    scale = table * groups / (kept + named)
    first = (me * table + sec * (tall * LANES)).astype(jnp.float32)
    found = over_rows([first + (q * LANES) + lane for q in range(batch)], jnp.maximum)
    for q in range(batch):
        top = jnp.max(found[q], axis=0, keepdims=True)
        weights_out[q:q + 1, :] = jnp.where(top > 0.0, top, old[pl.ds(sec * tall + q, 1), :]) * scale

    departed(all_but_one(result), rw_send.at[0])

    @pl.when(sec == last)
    def _():
        departed(result.at[pl.ds(0, sections - 1)], up_send.at[0])


def handed(rewards, weights, rewards_out, weights_out):
    rewards_out[...] = rewards[...]
    weights_out[...] = weights[...]


def on_device(
    features, ages, age_table, returns, owners, slots, norm_gain,
    w_gate, w_up, w_down, final_gain, reward_head, old_priority,
):
    sections, groups = lax.axis_size("section"), lax.axis_size("rows")
    rows, width = features.shape
    block = rows * groups // (MICRO * 2 * SIDE)
    rounds = MICRO // SIDE
    ff = w_gate.shape[2]
    even = ff // 256 * 256
    table = old_priority.shape[0]
    lines = table // LANES
    vmem = pl.BlockSpec(memory_space=pltpu.VMEM)
    far = pl.BlockSpec(memory_space=pl.ANY)
    bf16, f32, dma = jnp.bfloat16, jnp.float32, pltpu.SemaphoreType.DMA
    rewards, weights = pl.pallas_call(
        functools.partial(kernel, sections, groups),
        out_shape=(
            jax.ShapeDtypeStruct((1, rows // sections), f32),
            jax.ShapeDtypeStruct((lines // sections, LANES), f32),
        ),
        in_specs=[vmem] * 7 + [far] * 3 + [vmem] * 3,
        out_specs=(vmem, vmem),
        scratch_shapes=[
            pltpu.VMEM((ff, width), bf16),
            pltpu.VMEM((ff, width), bf16),
            pltpu.VMEM((ff, width), bf16),
            pltpu.VMEM((width, 2 * even + 256), bf16),
            pltpu.VMEM((MICRO, 2, block, width), bf16),
            pltpu.VMEM((MICRO, 2, SIDE, block, width), bf16),
            pltpu.VMEM((2 * SIDE * block, ff), bf16),
            pltpu.VMEM((MICRO, 2, SIDE, block, width), bf16),
            pltpu.VMEM((MICRO, 2, SIDE - 1, block, width), bf16),
            pltpu.VMEM((MICRO, 2, block, width), bf16),
            pltpu.VMEM((MICRO, 2, SIDE, block, width), bf16),
            pltpu.VMEM((rounds, 2, SIDE - 1, block, width), bf16),
            pltpu.VMEM((2, width), f32),
            pltpu.VMEM((2, rounds, block, LANES), f32),
            pltpu.VMEM((groups, 1, rows), f32),
            pltpu.VMEM((groups, rows, LANES), f32),
            pltpu.VMEM((groups, 2, rows), f32),
            pltpu.VMEM((groups, rows, LANES), f32),
            pltpu.VMEM((groups, 1, LANES), f32),
            pltpu.VMEM((groups, 1, LANES), f32),
            pltpu.VMEM((lines, LANES), f32),
            pltpu.VMEM((groups, 1, LANES), f32),
            dma((3,)),
            dma((1,)),
            dma((1,)), dma((RING, 2)),
            dma((1,)), dma((RING, 2)),
            dma((1,)), dma((MICRO, 2)),
            dma((rounds, 2)),
            dma((1,)), dma((1,)),
            dma((1,)), dma((1,)),
            dma((1,)), dma((1,)),
            dma((1,)), dma((1,)),
        ],
        compiler_params=pltpu.CompilerParams(
            collective_id=0, has_side_effects=True, vmem_limit_bytes=56 * 1024 * 1024
        ),
        name="refresh",
    )(
        features, ages.reshape(1, rows), age_table, returns.reshape(1, rows),
        owners.reshape(1, rows), slots.reshape(1, rows),
        norm_gain, w_gate[0].T, w_up[0].T, w_down[0],
        final_gain.reshape(-1, LANES), reward_head.reshape(-1, LANES),
        old_priority.reshape(lines, LANES),
    )
    rewards, weights = pl.pallas_call(
        handed, out_shape=tuple(jax.ShapeDtypeStruct(each.shape, f32) for each in (rewards, weights)),
        in_specs=[vmem, vmem], out_specs=(vmem, vmem), name="handed",
    )(rewards, weights)
    return rewards.reshape(-1), weights.reshape(-1)


def solution(mesh):
    placed = (
        P("rows", None),
        P("rows"),
        P(),
        P("rows"),
        P("rows", None),
        P("rows"),
        P("section", None),
        P("section", None, "rows"),
        P("section", None, "rows"),
        P("section", "rows", None),
        P(),
        P(),
        P("rows"),
    )
    return jax.shard_map(
        on_device,
        mesh=mesh,
        in_specs=placed,
        out_specs=(P(("rows", "section")), P(("rows", "section"))),
        check_vma=False,
    )
```

```python
import functools

import jax
import jax.numpy as jnp
from jax import lax
from jax.experimental import pallas as pl
from jax.experimental.pallas import tpu as pltpu
from jax.sharding import PartitionSpec as P

MICRO = 32
ENTER_AHEAD = 3
WORK_AHEAD = 2
RING = 4
SIDE = 4
MESH = pl.DeviceIdType.MESH
LANES = 128


def chunks(total, size):
    return [(at, min(size, total - at)) for at in range(0, total, size)]


def remote(src, dst, send_sem, recv_sem, where):
    return pltpu.make_async_remote_copy(
        src_ref=src, dst_ref=dst, send_sem=send_sem, recv_sem=recv_sem,
        device_id=where, device_id_type=MESH,
    )


def kernel(
    sections, groups,
    features, ages, age_table, returns, owners, slots, gain, w_gate, w_up, w_down,
    final_gain, head, old,
    rewards_out, weights_out,
    wg, wu, wd, w_both, state, gathered, hidden, part, part_in, line_out, line_in, last_in,
    final_row, reward_cols, marks, marks_wide, result, prio_wide, tops, shares, spare, sums,
    w_sem,
    in_send, ag_send, ag_recv, rs_send, rs_recv, ln_send, ln_recv, fn_recv,
    mk_send, mk_recv, up_send, up_recv, rw_send, rw_recv, sm_send, sm_recv,
):
    sec = lax.axis_index("section")
    me = lax.axis_index("rows")
    spot = (lax.rem(me, SIDE), me // SIDE)
    block, width = state.shape[2], state.shape[3]
    rows = features.shape[0]
    ff = hidden.shape[1]
    even = ff // 256 * 256
    rest = ff - even
    last = sections - 1
    rounds = MICRO // SIDE

    def step_on(axis, d):
        return lax.rem(spot[axis] + d, SIDE)

    def on_line(axis, index):
        return spot[1] * SIDE + index if axis == 0 else index * SIDE + spot[0]

    loads = [
        pltpu.make_async_copy(w_gate, wg, w_sem.at[0]),
        pltpu.make_async_copy(w_up, wu, w_sem.at[1]),
        pltpu.make_async_copy(w_down, wd, w_sem.at[2]),
    ]
    for load in loads:
        load.start()

    barrier = pltpu.get_barrier_semaphore()
    for j in range(1, groups):
        pl.semaphore_signal(barrier, inc=1, device_id={"rows": lax.rem(me + j, groups)}, device_id_type=MESH)
    for j in range(1, sections):
        pl.semaphore_signal(barrier, inc=1, device_id={"section": lax.rem(sec + j, sections)}, device_id_type=MESH)
    before = lax.rem(sec + last, sections)
    for axis in range(2):
        for d in range(1, SIDE):
            pl.semaphore_signal(
                barrier, inc=1, device_id={"section": before, "rows": on_line(axis, step_on(axis, d))}, device_id_type=MESH
            )

    marks[me] = (owners[...] * (old.shape[0] * LANES) + slots[...]).astype(jnp.float32)

    for i in range(final_gain.shape[0]):
        final_row[0:1, i * LANES:(i + 1) * LANES] = final_gain[i:i + 1, :]
        final_row[1:2, i * LANES:(i + 1) * LANES] = head[i:i + 1, :]

    @pl.when(sec == 0)
    def _():
        tall = jnp.transpose(jnp.broadcast_to(ages[...].astype(jnp.float32), (LANES, rows)))
        buckets = age_table.shape[0]
        onehot = (
            tall[:, :buckets] == lax.broadcasted_iota(jnp.int32, (rows, buckets), 1).astype(jnp.float32)
        ).astype(jnp.float32).astype(jnp.bfloat16)
        for at, size in chunks(width, 512):
            entry = features[:, at:at + size].astype(jnp.float32) + jnp.dot(
                onehot, age_table[:, at:at + size], preferred_element_type=jnp.float32
            )
            entry = entry.astype(jnp.bfloat16).reshape(2, rounds, block, size)
            for h in range(2):
                for k in range(rounds):
                    state[k * SIDE + spot[1 - h], h, :, at:at + size] = entry[h, k]

    def turned(load, flat, first):
        load.wait()
        for at in range(0, even, 256):
            w_both[:, first * even + at:first * even + at + 256] = jnp.transpose(flat[at:at + 256, :])
        w_both[:, 2 * even + first * LANES:2 * even + first * LANES + rest] = jnp.transpose(flat[even:ff, :])

    w_both[:, 2 * even:2 * even + 256] = jnp.zeros((width, 256), jnp.bfloat16)
    turned(loads[0], wg, 0)
    turned(loads[1], wu, 1)
    loads[2].wait()

    pl.semaphore_wait(barrier, groups - 1 + sections - 1 + 2 * (SIDE - 1))

    here = {"rows": lax.rem(me + 1, groups)}

    def arrived(ref, recv):
        remote(ref, ref, in_send.at[0], recv, here).wait_recv()

    def departed(ref, send):
        remote(ref, ref, send, ln_recv.at[0, 0], here).wait_send()

    def to_group(ref, send, recv, j):
        return remote(ref.at[me], ref.at[me], send.at[0], recv.at[0], {"rows": lax.rem(me + j, groups)})

    def all_but_one(ref):
        return ref.at[pl.ds(0, groups - 1)]

    def in_copy(k, h, d):
        t = k * SIDE + spot[1 - h]
        ref = state.at[t, h]
        return remote(ref, ref, in_send.at[0], ln_recv.at[t, h], {"rows": on_line(1 - h, step_on(1 - h, d))})

    def ag_copy(t, h, d):
        ref = gathered.at[t, h, spot[h]]
        return remote(ref, ref, ag_send.at[0], ag_recv.at[lax.rem(t, RING), h], {"rows": on_line(h, step_on(h, d))})

    def rs_copy(t, h, d):
        return remote(
            part.at[t, h, step_on(h, d)], part_in.at[t, h, d - 1], rs_send.at[0], rs_recv.at[lax.rem(t, RING), h],
            {"rows": on_line(h, step_on(h, d))},
        )

    def line_copy(t, h, d):
        return remote(
            line_out.at[t, h], line_in.at[t, h, spot[1 - h]], ln_send.at[0], ln_recv.at[t, h],
            {"section": jnp.minimum(sec + 1, last), "rows": on_line(1 - h, step_on(1 - h, d))},
        )

    def home_of(t):
        return lax.rem(t, SIDE)

    def last_copy(t, h, k):
        home = home_of(t)
        where = home * SIDE + k if h == 0 else k * SIDE + home
        slot = lax.rem(me - where + groups + groups - 1, groups)
        return remote(
            part.at[t, h, k], last_in.at[t // SIDE, h, slot], rs_send.at[0], fn_recv.at[t // SIDE, h], {"rows": where}
        )

    def normed(t, h):
        wide = state[t, h].astype(jnp.float32)
        scale = lax.rsqrt(jnp.mean(wide * wide, axis=-1, keepdims=True) + 1e-06)
        gathered[t, h, spot[h]] = (wide * scale * gain[...]).astype(jnp.bfloat16)

    def enter(t):
        for h in range(2):
            @pl.when(sec > 0)
            def _():
                arrived(line_in.at[t, h], ln_recv.at[t, h])
                total = line_in[t, h, 0].astype(jnp.float32)
                for i in range(1, SIDE):
                    total = total + line_in[t, h, i].astype(jnp.float32)
                state[t, h] = total.astype(jnp.bfloat16)

            @pl.when((sec == 0) & (spot[1 - h] != home_of(t)))
            def _():
                arrived(state.at[t, h], ln_recv.at[t, h])

            normed(t, h)
            for d in (2, 1, 3):
                ag_copy(t, h, d).start()

    def work(t):
        for h in range(2):
            foreign = (sec == 0) & (t == 0) & (spot[1 - h] > 0)

            @pl.when(foreign)
            def _():
                arrived(gathered.at[t, h], ag_recv.at[0, h])

            @pl.when(jnp.logical_not(foreign))
            def _():
                arrived(gathered.at[t, h, pl.ds(0, SIDE - 1)], ag_recv.at[lax.rem(t, RING), h])
        piece = gathered[t].reshape(2 * SIDE * block, width)
        for at in range(0, even, 256):
            gate = jnp.dot(piece, w_both[:, at:at + 256], preferred_element_type=jnp.float32)
            upper = jnp.dot(piece, w_both[:, even + at:even + at + 256], preferred_element_type=jnp.float32)
            hidden[:, at:at + 256] = (gate / (1.0 + jnp.exp(-gate)) * upper).astype(jnp.bfloat16)
        ends = jnp.dot(piece, w_both[:, 2 * even:2 * even + 256], preferred_element_type=jnp.float32)
        gate, upper = ends[:, :rest], ends[:, LANES:LANES + rest]
        hidden[:, even:ff] = (gate / (1.0 + jnp.exp(-gate)) * upper).astype(jnp.bfloat16)
        units = hidden[...]
        for at, size in chunks(width, 256):
            down = jnp.dot(units, wd[:, at:at + size], preferred_element_type=jnp.float32)
            part[t, :, :, :, at:at + size] = down.astype(jnp.bfloat16).reshape(2, SIDE, block, size)

        @pl.when(sec < last)
        def _():
            for h in range(2):
                for d in (2, 1, 3):
                    rs_copy(t, h, d).start()

        @pl.when(sec == last)
        def _():
            for h in range(2):
                for k in range(SIDE):
                    @pl.when((spot[h] != k) | (spot[1 - h] != home_of(t)))
                    def _():
                        last_copy(t, h, k).start()

    def leave(t):
        home = home_of(t)
        for h in range(2):
            total = part[t, h, spot[h]].astype(jnp.float32)
            total = total + jnp.where(spot[1 - h] == home, state[t, h].astype(jnp.float32), 0.0)
            arrived(part_in.at[t, h], rs_recv.at[lax.rem(t, RING), h])
            for d in range(1, SIDE):
                total = total + part_in[t, h, d - 1].astype(jnp.float32)
            line_out[t, h] = total.astype(jnp.bfloat16)

            for d in (0, 2, 1, 3):
                line_copy(t, h, d).start()

    def finish(t):
        k = t // SIDE
        for h in range(2):
            @pl.when(spot[1 - h] == home_of(t))
            def _():
                total = state[t, h].astype(jnp.float32) + part[t, h, spot[h]].astype(jnp.float32)
                arrived(last_in.at[k, h], fn_recv.at[k, h])
                for j in range(groups - 1):
                    total = total + last_in[k, h, j].astype(jnp.float32)
                wide = total.astype(jnp.bfloat16).astype(jnp.float32)
                scale = lax.rsqrt(jnp.mean(wide * wide, axis=-1, keepdims=True) + 1e-06)
                value = jnp.sum(wide * scale * final_row[0:1] * final_row[1:2], axis=-1, keepdims=True)
                reward_cols[h, k] = jnp.broadcast_to(value, (block, LANES))

    @pl.when(sec == 0)
    def _():
        for h in range(2):
            @pl.when(spot[1 - h] == 0)
            def _():
                normed(0, h)
                ref = gathered.at[0, h, spot[h]]
                for j in range(1, groups):
                    remote(ref, ref, ag_send.at[0], ag_recv.at[0, h], {"rows": lax.rem(me + j, groups)}).start()
        for k in range(rounds):
            for h in range(2):
                @pl.when((spot[1 - h] > 0) | (k > 0))
                def _():
                    for d in (2, 1, 3):
                        in_copy(k, h, d).start()

    for j in range(1, groups):
        to_group(marks, mk_send, mk_recv, j).start()

    lines = old.shape[0]
    table = lines * LANES
    tall = lines // sections
    batch = 4
    lane = lax.broadcasted_iota(jnp.int32, (1, LANES), 1).astype(jnp.float32)

    def over_rows(names, join):
        def one(r, best):
            best = list(best)
            for i in range(0, rows, 8):
                mark = marks_wide[r, i:i + 8, :]
                value = prio_wide[r, i:i + 8, :]
                for q in range(batch):
                    best[q] = join(best[q], jnp.where(mark == names[q], value, 0.0))
            return tuple(best)

        return lax.fori_loop(0, groups, one, tuple(jnp.zeros((8, LANES), jnp.float32) for _ in range(batch)))

    def count():
        arrived(all_but_one(marks), mk_recv.at[0])
        for r in range(groups):
            marks_wide[r] = jnp.transpose(jnp.broadcast_to(marks[r], (LANES, rows)))
            prio_wide[r] = jnp.ones((rows, LANES), jnp.float32)

        def by_row(g, carry):
            found = over_rows([marks[g * batch + q] for q in range(batch)], jnp.add)
            for q in range(batch):
                shares[g * batch + q] = 1.0 / jnp.sum(found[q], axis=0, keepdims=True)
            return carry

        lax.fori_loop(0, groups // batch, by_row, 0)

        def by_entry(g, carry):
            first = (me * table + g * (batch * LANES)).astype(jnp.float32)
            found = over_rows([first + (q * LANES) + lane for q in range(batch)], jnp.add)
            for q in range(batch):
                at = pl.ds(g * batch + q, 1)
                spare[at, :] = jnp.where(jnp.sum(found[q], axis=0, keepdims=True) > 0.0, 0.0, old[at, :])
            return carry

        lax.fori_loop(0, lines // batch, by_entry, 0)
        subtotal = jnp.sum(jnp.sum(spare[...], axis=0, keepdims=True), axis=1, keepdims=True)
        sums[me] = jnp.broadcast_to(subtotal, (1, LANES))
        for j in range(1, groups):
            to_group(sums, sm_send, sm_recv, j).start()

    @pl.when(sec >= sections // 2)
    def _():
        count()

    def step(i, carry):
        t = i - ENTER_AHEAD

        @pl.when((sec == last) & (t >= 0))
        def _():
            finish(t)

        @pl.when((sec < last) & (t >= 0))
        def _():
            leave(t)

        @pl.when((i + head_start < MICRO) & ((sec > 0) | (i + head_start > 0)))
        def _():
            enter(i + head_start)

        @pl.when((t + WORK_AHEAD >= 0) & (t + WORK_AHEAD < MICRO))
        def _():
            work(t + WORK_AHEAD)

        return carry

    head_start = jnp.where(sec == 0, 1, 0)

    lax.fori_loop(0, MICRO + ENTER_AHEAD, step, 0)

    @pl.when(sec < sections // 2)
    def _():
        count()

    def up_copy(j):
        return remote(result.at[me], result.at[me], up_send.at[0], up_recv.at[0], {"section": last - j})

    @pl.when(sec == last)
    def _():
        square = reward_cols[...].reshape(rows, LANES)
        on_diagonal = lax.broadcasted_iota(jnp.int32, (rows, rows), 0) == lax.broadcasted_iota(jnp.int32, (rows, rows), 1)
        row = jnp.sum(jnp.where(on_diagonal, square, 0.0), axis=0, keepdims=True)
        priority = jnp.exp(0.6 * jnp.log(jnp.abs(row - returns[...]) + 0.05))
        result[me, 0:1] = row
        result[me, 1:2] = priority
        for j in range(1, sections):
            up_copy(j).start()


    @pl.when(sec > 0)
    def _():
        departed(part_in, ag_send.at[0])


    @pl.when(sec < last)
    def _():
        departed(part_in, rs_send.at[0])

    @pl.when(sec == last)
    def _():
        departed(part.at[pl.ds(0, MICRO - rounds // SIDE)], rs_send.at[0])

    departed(all_but_one(marks), mk_send.at[0])

    @pl.when(sec == 0)
    def _():
        departed(part_in.at[pl.ds(0, MICRO - 1)], ag_send.at[0])
        departed(part_in.at[pl.ds(0, rounds - 1)], in_send.at[0])
        for h in range(2):
            @pl.when(spot[1 - h] == 0)
            def _():
                departed(last_in.at[0, 0], ag_send.at[0])

            @pl.when(spot[1 - h] > 0)
            def _():
                departed(part_in.at[0, 0], in_send.at[0])

    arrived(all_but_one(sums), sm_recv.at[0])
    departed(all_but_one(sums), sm_send.at[0])
    kept = sums[0]
    for r in range(1, groups):
        kept = kept + sums[r]

    @pl.when(sec < last)
    def _():
        departed(line_in, ln_send.at[0])
        arrived(result.at[me], up_recv.at[0])

    for j in range(1, groups):
        to_group(result, rw_send, rw_recv, j).start()

    mine = result[me, 0:1]
    share = rows // sections
    picked = mine[:, 0:share]
    for s in range(1, sections):
        picked = jnp.where(sec == s, mine[:, s * share:(s + 1) * share], picked)
    rewards_out[...] = picked

    arrived(all_but_one(result), rw_recv.at[0])
    for r in range(groups):
        prio_wide[r] = jnp.transpose(jnp.broadcast_to(result[r, 1:2], (LANES, rows)))

    def by_row(g, carry):
        found = over_rows([marks[g * batch + q] for q in range(batch)], jnp.maximum)
        for q in range(batch):
            tops[g * batch + q] = jnp.max(found[q], axis=0, keepdims=True) * shares[g * batch + q]
        return carry

    lax.fori_loop(0, groups // batch, by_row, 0)
    named = jnp.sum(jnp.sum(tops[...], axis=0), axis=1, keepdims=True)
    scale = table * groups / (kept + named)
    first = (me * table + sec * (tall * LANES)).astype(jnp.float32)
    found = over_rows([first + (q * LANES) + lane for q in range(batch)], jnp.maximum)
    for q in range(batch):
        top = jnp.max(found[q], axis=0, keepdims=True)
        weights_out[q:q + 1, :] = jnp.where(top > 0.0, top, old[pl.ds(sec * tall + q, 1), :]) * scale

    departed(all_but_one(result), rw_send.at[0])

    @pl.when(sec == last)
    def _():
        departed(result.at[pl.ds(0, sections - 1)], up_send.at[0])


def handed(rewards, weights, rewards_out, weights_out):
    rewards_out[...] = rewards[...]
    weights_out[...] = weights[...]


def on_device(
    features, ages, age_table, returns, owners, slots, norm_gain,
    w_gate, w_up, w_down, final_gain, reward_head, old_priority,
):
    sections, groups = lax.axis_size("section"), lax.axis_size("rows")
    rows, width = features.shape
    block = rows * groups // (MICRO * 2 * SIDE)
    rounds = MICRO // SIDE
    ff = w_gate.shape[2]
    even = ff // 256 * 256
    table = old_priority.shape[0]
    lines = table // LANES
    vmem = pl.BlockSpec(memory_space=pltpu.VMEM)
    far = pl.BlockSpec(memory_space=pl.ANY)
    bf16, f32, dma = jnp.bfloat16, jnp.float32, pltpu.SemaphoreType.DMA
    rewards, weights = pl.pallas_call(
        functools.partial(kernel, sections, groups),
        out_shape=(
            jax.ShapeDtypeStruct((1, rows // sections), f32),
            jax.ShapeDtypeStruct((lines // sections, LANES), f32),
        ),
        in_specs=[vmem] * 7 + [far] * 3 + [vmem] * 3,
        out_specs=(vmem, vmem),
        scratch_shapes=[
            pltpu.VMEM((ff, width), bf16),
            pltpu.VMEM((ff, width), bf16),
            pltpu.VMEM((ff, width), bf16),
            pltpu.VMEM((width, 2 * even + 256), bf16),
            pltpu.VMEM((MICRO, 2, block, width), bf16),
            pltpu.VMEM((MICRO, 2, SIDE, block, width), bf16),
            pltpu.VMEM((2 * SIDE * block, ff), bf16),
            pltpu.VMEM((MICRO, 2, SIDE, block, width), bf16),
            pltpu.VMEM((MICRO, 2, SIDE - 1, block, width), bf16),
            pltpu.VMEM((MICRO, 2, block, width), bf16),
            pltpu.VMEM((MICRO, 2, SIDE, block, width), bf16),
            pltpu.VMEM((rounds, 2, groups - 1, block, width), bf16),
            pltpu.VMEM((2, width), f32),
            pltpu.VMEM((2, rounds, block, LANES), f32),
            pltpu.VMEM((groups, 1, rows), f32),
            pltpu.VMEM((groups, rows, LANES), f32),
            pltpu.VMEM((groups, 2, rows), f32),
            pltpu.VMEM((groups, rows, LANES), f32),
            pltpu.VMEM((groups, 1, LANES), f32),
            pltpu.VMEM((groups, 1, LANES), f32),
            pltpu.VMEM((lines, LANES), f32),
            pltpu.VMEM((groups, 1, LANES), f32),
            dma((3,)),
            dma((1,)),
            dma((1,)), dma((RING, 2)),
            dma((1,)), dma((RING, 2)),
            dma((1,)), dma((MICRO, 2)),
            dma((rounds, 2)),
            dma((1,)), dma((1,)),
            dma((1,)), dma((1,)),
            dma((1,)), dma((1,)),
            dma((1,)), dma((1,)),
        ],
        compiler_params=pltpu.CompilerParams(
            collective_id=0, has_side_effects=True, vmem_limit_bytes=56 * 1024 * 1024
        ),
        name="refresh",
    )(
        features, ages.reshape(1, rows), age_table, returns.reshape(1, rows),
        owners.reshape(1, rows), slots.reshape(1, rows),
        norm_gain, w_gate[0].T, w_up[0].T, w_down[0],
        final_gain.reshape(-1, LANES), reward_head.reshape(-1, LANES),
        old_priority.reshape(lines, LANES),
    )
    rewards, weights = pl.pallas_call(
        handed, out_shape=tuple(jax.ShapeDtypeStruct(each.shape, f32) for each in (rewards, weights)),
        in_specs=[vmem, vmem], out_specs=(vmem, vmem), name="handed",
    )(rewards, weights)
    return rewards.reshape(-1), weights.reshape(-1)


def solution(mesh):
    placed = (
        P("rows", None),
        P("rows"),
        P(),
        P("rows"),
        P("rows", None),
        P("rows"),
        P("section", None),
        P("section", None, "rows"),
        P("section", None, "rows"),
        P("section", "rows", None),
        P(),
        P(),
        P("rows"),
    )
    return jax.shard_map(
        on_device,
        mesh=mesh,
        in_specs=placed,
        out_specs=(P(("rows", "section")), P(("rows", "section"))),
        check_vma=False,
    )
```

```python
import functools

import jax
import jax.numpy as jnp
from jax import lax
from jax.experimental import pallas as pl
from jax.experimental.pallas import tpu as pltpu
from jax.sharding import PartitionSpec as P

MICRO = 32
ENTER_AHEAD = 3
WORK_AHEAD = 2
RING = 4
SIDE = 4
MESH = pl.DeviceIdType.MESH
LANES = 128


def chunks(total, size):
    return [(at, min(size, total - at)) for at in range(0, total, size)]


def remote(src, dst, send_sem, recv_sem, where):
    return pltpu.make_async_remote_copy(
        src_ref=src, dst_ref=dst, send_sem=send_sem, recv_sem=recv_sem,
        device_id=where, device_id_type=MESH,
    )


def kernel(
    sections, groups,
    features, ages, age_table, returns, owners, slots, gain, w_gate, w_up, w_down,
    final_gain, head, old,
    rewards_out, weights_out,
    wg, wu, wd, w_both, state, gathered, hidden, part, part_in, line_out, line_in, last_in,
    final_row, reward_cols, marks, marks_wide, result, prio_wide, tops, shares, spare, sums,
    w_sem,
    in_send, ag_send, ag_recv, rs_send, rs_recv, ln_send, ln_recv, fn_recv,
    mk_send, mk_recv, up_send, up_recv, rw_send, rw_recv, sm_send, sm_recv,
):
    sec = lax.axis_index("section")
    me = lax.axis_index("rows")
    spot = (lax.rem(me, SIDE), me // SIDE)
    block, width = state.shape[2], state.shape[3]
    rows = features.shape[0]
    ff = hidden.shape[1]
    even = ff // 256 * 256
    rest = ff - even
    last = sections - 1
    rounds = MICRO // SIDE

    def step_on(axis, d):
        return lax.rem(spot[axis] + d, SIDE)

    def on_line(axis, index):
        return spot[1] * SIDE + index if axis == 0 else index * SIDE + spot[0]

    loads = [
        pltpu.make_async_copy(w_gate, wg, w_sem.at[0]),
        pltpu.make_async_copy(w_up, wu, w_sem.at[1]),
        pltpu.make_async_copy(w_down, wd, w_sem.at[2]),
    ]
    for load in loads:
        load.start()

    barrier = pltpu.get_barrier_semaphore()
    for j in range(1, groups):
        pl.semaphore_signal(barrier, inc=1, device_id={"rows": lax.rem(me + j, groups)}, device_id_type=MESH)
    for j in range(1, sections):
        pl.semaphore_signal(barrier, inc=1, device_id={"section": lax.rem(sec + j, sections)}, device_id_type=MESH)
    before = lax.rem(sec + last, sections)
    for axis in range(2):
        for d in range(1, SIDE):
            pl.semaphore_signal(
                barrier, inc=1, device_id={"section": before, "rows": on_line(axis, step_on(axis, d))}, device_id_type=MESH
            )

    marks[me] = (owners[...] * (old.shape[0] * LANES) + slots[...]).astype(jnp.float32)

    for i in range(final_gain.shape[0]):
        final_row[0:1, i * LANES:(i + 1) * LANES] = final_gain[i:i + 1, :]
        final_row[1:2, i * LANES:(i + 1) * LANES] = head[i:i + 1, :]

    @pl.when(sec == 0)
    def _():
        tall = jnp.transpose(jnp.broadcast_to(ages[...].astype(jnp.float32), (LANES, rows)))
        buckets = age_table.shape[0]
        onehot = (
            tall[:, :buckets] == lax.broadcasted_iota(jnp.int32, (rows, buckets), 1).astype(jnp.float32)
        ).astype(jnp.float32).astype(jnp.bfloat16)
        for at, size in chunks(width, 512):
            entry = features[:, at:at + size].astype(jnp.float32) + jnp.dot(
                onehot, age_table[:, at:at + size], preferred_element_type=jnp.float32
            )
            entry = entry.astype(jnp.bfloat16).reshape(2, rounds, block, size)
            for h in range(2):
                for k in range(rounds):
                    state[k * SIDE + spot[1 - h], h, :, at:at + size] = entry[h, k]

    def turned(load, flat, first):
        load.wait()
        for at in range(0, even, 256):
            w_both[:, first * even + at:first * even + at + 256] = jnp.transpose(flat[at:at + 256, :])
        w_both[:, 2 * even + first * LANES:2 * even + first * LANES + rest] = jnp.transpose(flat[even:ff, :])

    w_both[:, 2 * even:2 * even + 256] = jnp.zeros((width, 256), jnp.bfloat16)
    turned(loads[0], wg, 0)
    turned(loads[1], wu, 1)
    loads[2].wait()

    pl.semaphore_wait(barrier, groups - 1 + sections - 1 + 2 * (SIDE - 1))

    here = {"rows": lax.rem(me + 1, groups)}

    def arrived(ref, recv):
        remote(ref, ref, in_send.at[0], recv, here).wait_recv()

    def departed(ref, send):
        remote(ref, ref, send, ln_recv.at[0, 0], here).wait_send()

    def to_group(ref, send, recv, j):
        return remote(ref.at[me], ref.at[me], send.at[0], recv.at[0], {"rows": lax.rem(me + j, groups)})

    def all_but_one(ref):
        return ref.at[pl.ds(0, groups - 1)]

    def in_copy(k, h, d):
        t = k * SIDE + spot[1 - h]
        ref = state.at[t, h]
        return remote(ref, ref, in_send.at[0], ln_recv.at[t, h], {"rows": on_line(1 - h, step_on(1 - h, d))})

    def ag_copy(t, h, d):
        ref = gathered.at[t, h, spot[h]]
        return remote(ref, ref, ag_send.at[0], ag_recv.at[lax.rem(t, RING), h], {"rows": on_line(h, step_on(h, d))})

    def rs_copy(t, h, d):
        return remote(
            part.at[t, h, step_on(h, d)], part_in.at[t, h, d - 1], rs_send.at[0], rs_recv.at[lax.rem(t, RING), h],
            {"rows": on_line(h, step_on(h, d))},
        )

    def line_copy(t, h, d):
        return remote(
            line_out.at[t, h], line_in.at[t, h, spot[1 - h]], ln_send.at[0], ln_recv.at[t, h],
            {"section": jnp.minimum(sec + 1, last), "rows": on_line(1 - h, step_on(1 - h, d))},
        )

    def home_of(t):
        return lax.rem(t, SIDE)

    def last_copy(t, h):
        home = home_of(t)
        d = lax.rem(home + SIDE - spot[1 - h] + SIDE - 1, SIDE)
        k = t // SIDE
        return remote(
            line_out.at[t, h], last_in.at[k, h, d], ln_send.at[0], fn_recv.at[k, h],
            {"rows": on_line(1 - h, home)},
        )

    def normed(t, h):
        wide = state[t, h].astype(jnp.float32)
        scale = lax.rsqrt(jnp.mean(wide * wide, axis=-1, keepdims=True) + 1e-06)
        gathered[t, h, spot[h]] = (wide * scale * gain[...]).astype(jnp.bfloat16)

    def enter(t):
        for h in range(2):
            @pl.when(sec > 0)
            def _():
                arrived(line_in.at[t, h], ln_recv.at[t, h])
                total = line_in[t, h, 0].astype(jnp.float32)
                for i in range(1, SIDE):
                    total = total + line_in[t, h, i].astype(jnp.float32)
                state[t, h] = total.astype(jnp.bfloat16)

            @pl.when((sec == 0) & (spot[1 - h] != home_of(t)))
            def _():
                arrived(state.at[t, h], ln_recv.at[t, h])

            normed(t, h)
            for d in (2, 1, 3):
                ag_copy(t, h, d).start()

    def work(t):
        for h in range(2):
            foreign = (sec == 0) & (t == 0) & (spot[1 - h] > 0)

            @pl.when(foreign)
            def _():
                arrived(gathered.at[t, h], ag_recv.at[0, h])

            @pl.when(jnp.logical_not(foreign))
            def _():
                arrived(gathered.at[t, h, pl.ds(0, SIDE - 1)], ag_recv.at[lax.rem(t, RING), h])
        piece = gathered[t].reshape(2 * SIDE * block, width)
        for at in range(0, even, 256):
            gate = jnp.dot(piece, w_both[:, at:at + 256], preferred_element_type=jnp.float32)
            upper = jnp.dot(piece, w_both[:, even + at:even + at + 256], preferred_element_type=jnp.float32)
            hidden[:, at:at + 256] = (gate / (1.0 + jnp.exp(-gate)) * upper).astype(jnp.bfloat16)
        ends = jnp.dot(piece, w_both[:, 2 * even:2 * even + 256], preferred_element_type=jnp.float32)
        gate, upper = ends[:, :rest], ends[:, LANES:LANES + rest]
        hidden[:, even:ff] = (gate / (1.0 + jnp.exp(-gate)) * upper).astype(jnp.bfloat16)
        units = hidden[...]
        for at, size in chunks(width, 256):
            down = jnp.dot(units, wd[:, at:at + size], preferred_element_type=jnp.float32)
            part[t, :, :, :, at:at + size] = down.astype(jnp.bfloat16).reshape(2, SIDE, block, size)
        for d in (2, 1, 3):
            for h in range(2):
                rs_copy(t, h, d).start()

    def leave(t):
        home = home_of(t)
        for h in range(2):
            total = part[t, h, spot[h]].astype(jnp.float32)
            total = total + jnp.where(spot[1 - h] == home, state[t, h].astype(jnp.float32), 0.0)
            arrived(part_in.at[t, h], rs_recv.at[lax.rem(t, RING), h])
            for d in range(1, SIDE):
                total = total + part_in[t, h, d - 1].astype(jnp.float32)
            line_out[t, h] = total.astype(jnp.bfloat16)

            @pl.when(sec < last)
            def _():
                for d in (0, 2, 1, 3):
                    line_copy(t, h, d).start()

            @pl.when((sec == last) & (spot[1 - h] != home))
            def _():
                last_copy(t, h).start()

    def finish(t):
        k = t // SIDE
        for h in range(2):
            @pl.when(spot[1 - h] == home_of(t))
            def _():
                total = line_out[t, h].astype(jnp.float32)
                arrived(last_in.at[k, h], fn_recv.at[k, h])
                for d in range(1, SIDE):
                    total = total + last_in[k, h, d - 1].astype(jnp.float32)
                wide = total.astype(jnp.bfloat16).astype(jnp.float32)
                scale = lax.rsqrt(jnp.mean(wide * wide, axis=-1, keepdims=True) + 1e-06)
                value = jnp.sum(wide * scale * final_row[0:1] * final_row[1:2], axis=-1, keepdims=True)
                reward_cols[h, k] = jnp.broadcast_to(value, (block, LANES))

    @pl.when(sec == 0)
    def _():
        for h in range(2):
            @pl.when(spot[1 - h] == 0)
            def _():
                normed(0, h)
                ref = gathered.at[0, h, spot[h]]
                for j in range(1, groups):
                    remote(ref, ref, ag_send.at[0], ag_recv.at[0, h], {"rows": lax.rem(me + j, groups)}).start()
        for k in range(rounds):
            for h in range(2):
                @pl.when((spot[1 - h] > 0) | (k > 0))
                def _():
                    for d in (2, 1, 3):
                        in_copy(k, h, d).start()

    for j in range(1, groups):
        to_group(marks, mk_send, mk_recv, j).start()

    lines = old.shape[0]
    table = lines * LANES
    tall = lines // sections
    batch = 4
    lane = lax.broadcasted_iota(jnp.int32, (1, LANES), 1).astype(jnp.float32)

    def over_rows(names, join):
        def one(r, best):
            best = list(best)
            for i in range(0, rows, 8):
                mark = marks_wide[r, i:i + 8, :]
                value = prio_wide[r, i:i + 8, :]
                for q in range(batch):
                    best[q] = join(best[q], jnp.where(mark == names[q], value, 0.0))
            return tuple(best)

        return lax.fori_loop(0, groups, one, tuple(jnp.zeros((8, LANES), jnp.float32) for _ in range(batch)))

    def count():
        arrived(all_but_one(marks), mk_recv.at[0])
        for r in range(groups):
            marks_wide[r] = jnp.transpose(jnp.broadcast_to(marks[r], (LANES, rows)))
            prio_wide[r] = jnp.ones((rows, LANES), jnp.float32)

        def by_row(g, carry):
            found = over_rows([marks[g * batch + q] for q in range(batch)], jnp.add)
            for q in range(batch):
                shares[g * batch + q] = 1.0 / jnp.sum(found[q], axis=0, keepdims=True)
            return carry

        lax.fori_loop(0, groups // batch, by_row, 0)

        def by_entry(g, carry):
            first = (me * table + g * (batch * LANES)).astype(jnp.float32)
            found = over_rows([first + (q * LANES) + lane for q in range(batch)], jnp.add)
            for q in range(batch):
                at = pl.ds(g * batch + q, 1)
                spare[at, :] = jnp.where(jnp.sum(found[q], axis=0, keepdims=True) > 0.0, 0.0, old[at, :])
            return carry

        lax.fori_loop(0, lines // batch, by_entry, 0)
        subtotal = jnp.sum(jnp.sum(spare[...], axis=0, keepdims=True), axis=1, keepdims=True)
        sums[me] = jnp.broadcast_to(subtotal, (1, LANES))
        for j in range(1, groups):
            to_group(sums, sm_send, sm_recv, j).start()

    @pl.when(sec >= sections // 2)
    def _():
        count()

    def step(i, carry):
        t = i - ENTER_AHEAD

        @pl.when((sec == last) & (t >= 2))
        def _():
            finish(t - 2)

        @pl.when(t >= 0)
        def _():
            leave(t)

        @pl.when((i + head_start < MICRO) & ((sec > 0) | (i + head_start > 0)))
        def _():
            enter(i + head_start)

        @pl.when((t + WORK_AHEAD >= 0) & (t + WORK_AHEAD < MICRO))
        def _():
            work(t + WORK_AHEAD)

        return carry

    head_start = jnp.where(sec == 0, 1, 0)

    lax.fori_loop(0, MICRO + ENTER_AHEAD, step, 0)

    @pl.when(sec < sections // 2)
    def _():
        count()

    def up_copy(j):
        return remote(result.at[me], result.at[me], up_send.at[0], up_recv.at[0], {"section": last - j})

    @pl.when(sec == last)
    def _():
        finish(MICRO - 2)
        finish(MICRO - 1)
        square = reward_cols[...].reshape(rows, LANES)
        on_diagonal = lax.broadcasted_iota(jnp.int32, (rows, rows), 0) == lax.broadcasted_iota(jnp.int32, (rows, rows), 1)
        row = jnp.sum(jnp.where(on_diagonal, square, 0.0), axis=0, keepdims=True)
        priority = jnp.exp(0.6 * jnp.log(jnp.abs(row - returns[...]) + 0.05))
        result[me, 0:1] = row
        result[me, 1:2] = priority
        for j in range(1, sections):
            up_copy(j).start()


    @pl.when(sec > 0)
    def _():
        departed(part_in, ag_send.at[0])

    departed(part_in, rs_send.at[0])
    departed(all_but_one(marks), mk_send.at[0])

    @pl.when(sec == 0)
    def _():
        departed(part_in.at[pl.ds(0, MICRO - 1)], ag_send.at[0])
        departed(part_in.at[pl.ds(0, rounds - 1)], in_send.at[0])
        for h in range(2):
            @pl.when(spot[1 - h] == 0)
            def _():
                departed(part_in.at[pl.ds(0, 5), 0], ag_send.at[0])

            @pl.when(spot[1 - h] > 0)
            def _():
                departed(part_in.at[0, 0], in_send.at[0])

    arrived(all_but_one(sums), sm_recv.at[0])
    departed(all_but_one(sums), sm_send.at[0])
    kept = sums[0]
    for r in range(1, groups):
        kept = kept + sums[r]

    @pl.when(sec < last)
    def _():
        departed(line_in, ln_send.at[0])
        arrived(result.at[me], up_recv.at[0])

    for j in range(1, groups):
        to_group(result, rw_send, rw_recv, j).start()

    @pl.when(sec == last)
    def _():
        departed(part_in.at[pl.ds(0, rounds)], ln_send.at[0])

    mine = result[me, 0:1]
    share = rows // sections
    picked = mine[:, 0:share]
    for s in range(1, sections):
        picked = jnp.where(sec == s, mine[:, s * share:(s + 1) * share], picked)
    rewards_out[...] = picked

    arrived(all_but_one(result), rw_recv.at[0])
    for r in range(groups):
        prio_wide[r] = jnp.transpose(jnp.broadcast_to(result[r, 1:2], (LANES, rows)))

    def by_row(g, carry):
        found = over_rows([marks[g * batch + q] for q in range(batch)], jnp.maximum)
        for q in range(batch):
            tops[g * batch + q] = jnp.max(found[q], axis=0, keepdims=True) * shares[g * batch + q]
        return carry

    lax.fori_loop(0, groups // batch, by_row, 0)
    named = jnp.sum(jnp.sum(tops[...], axis=0), axis=1, keepdims=True)
    scale = table * groups / (kept + named)
    first = (me * table + sec * (tall * LANES)).astype(jnp.float32)
    found = over_rows([first + (q * LANES) + lane for q in range(batch)], jnp.maximum)
    for q in range(batch):
        top = jnp.max(found[q], axis=0, keepdims=True)
        weights_out[q:q + 1, :] = jnp.where(top > 0.0, top, old[pl.ds(sec * tall + q, 1), :]) * scale

    departed(all_but_one(result), rw_send.at[0])

    @pl.when(sec == last)
    def _():
        departed(result.at[pl.ds(0, sections - 1)], up_send.at[0])


def handed(rewards, weights, rewards_out, weights_out):
    rewards_out[...] = rewards[...]
    weights_out[...] = weights[...]


def on_device(
    features, ages, age_table, returns, owners, slots, norm_gain,
    w_gate, w_up, w_down, final_gain, reward_head, old_priority,
):
    sections, groups = lax.axis_size("section"), lax.axis_size("rows")
    rows, width = features.shape
    block = rows * groups // (MICRO * 2 * SIDE)
    rounds = MICRO // SIDE
    ff = w_gate.shape[2]
    even = ff // 256 * 256
    table = old_priority.shape[0]
    lines = table // LANES
    vmem = pl.BlockSpec(memory_space=pltpu.VMEM)
    far = pl.BlockSpec(memory_space=pl.ANY)
    bf16, f32, dma = jnp.bfloat16, jnp.float32, pltpu.SemaphoreType.DMA
    rewards, weights = pl.pallas_call(
        functools.partial(kernel, sections, groups),
        out_shape=(
            jax.ShapeDtypeStruct((1, rows // sections), f32),
            jax.ShapeDtypeStruct((lines // sections, LANES), f32),
        ),
        in_specs=[vmem] * 7 + [far] * 3 + [vmem] * 3,
        out_specs=(vmem, vmem),
        scratch_shapes=[
            pltpu.VMEM((ff, width), bf16),
            pltpu.VMEM((ff, width), bf16),
            pltpu.VMEM((ff, width), bf16),
            pltpu.VMEM((width, 2 * even + 256), bf16),
            pltpu.VMEM((MICRO, 2, block, width), bf16),
            pltpu.VMEM((MICRO, 2, SIDE, block, width), bf16),
            pltpu.VMEM((2 * SIDE * block, ff), bf16),
            pltpu.VMEM((MICRO, 2, SIDE, block, width), bf16),
            pltpu.VMEM((MICRO, 2, SIDE - 1, block, width), bf16),
            pltpu.VMEM((MICRO, 2, block, width), bf16),
            pltpu.VMEM((MICRO, 2, SIDE, block, width), bf16),
            pltpu.VMEM((rounds, 2, SIDE - 1, block, width), bf16),
            pltpu.VMEM((2, width), f32),
            pltpu.VMEM((2, rounds, block, LANES), f32),
            pltpu.VMEM((groups, 1, rows), f32),
            pltpu.VMEM((groups, rows, LANES), f32),
            pltpu.VMEM((groups, 2, rows), f32),
            pltpu.VMEM((groups, rows, LANES), f32),
            pltpu.VMEM((groups, 1, LANES), f32),
            pltpu.VMEM((groups, 1, LANES), f32),
            pltpu.VMEM((lines, LANES), f32),
            pltpu.VMEM((groups, 1, LANES), f32),
            dma((3,)),
            dma((1,)),
            dma((1,)), dma((RING, 2)),
            dma((1,)), dma((RING, 2)),
            dma((1,)), dma((MICRO, 2)),
            dma((rounds, 2)),
            dma((1,)), dma((1,)),
            dma((1,)), dma((1,)),
            dma((1,)), dma((1,)),
            dma((1,)), dma((1,)),
        ],
        compiler_params=pltpu.CompilerParams(
            collective_id=0, has_side_effects=True, vmem_limit_bytes=56 * 1024 * 1024
        ),
        name="refresh",
    )(
        features, ages.reshape(1, rows), age_table, returns.reshape(1, rows),
        owners.reshape(1, rows), slots.reshape(1, rows),
        norm_gain, w_gate[0].T, w_up[0].T, w_down[0],
        final_gain.reshape(-1, LANES), reward_head.reshape(-1, LANES),
        old_priority.reshape(lines, LANES),
    )
    rewards, weights = pl.pallas_call(
        handed, out_shape=tuple(jax.ShapeDtypeStruct(each.shape, f32) for each in (rewards, weights)),
        in_specs=[vmem, vmem], out_specs=(vmem, vmem), name="handed",
    )(rewards, weights)
    return rewards.reshape(-1), weights.reshape(-1)


def solution(mesh):
    placed = (
        P("rows", None),
        P("rows"),
        P(),
        P("rows"),
        P("rows", None),
        P("rows"),
        P("section", None),
        P("section", None, "rows"),
        P("section", None, "rows"),
        P("section", "rows", None),
        P(),
        P(),
        P("rows"),
    )
    return jax.shard_map(
        on_device,
        mesh=mesh,
        in_specs=placed,
        out_specs=(P(("rows", "section")), P(("rows", "section"))),
        check_vma=False,
    )
```

```python
import functools

import jax
import jax.numpy as jnp
from jax import lax
from jax.experimental import pallas as pl
from jax.experimental.pallas import tpu as pltpu
from jax.sharding import PartitionSpec as P

MICRO = 32
ENTER_AHEAD = 3
WORK_AHEAD = 2
RING = 4
SIDE = 4
MESH = pl.DeviceIdType.MESH
LANES = 128


def chunks(total, size):
    return [(at, min(size, total - at)) for at in range(0, total, size)]


def remote(src, dst, send_sem, recv_sem, where):
    return pltpu.make_async_remote_copy(
        src_ref=src, dst_ref=dst, send_sem=send_sem, recv_sem=recv_sem,
        device_id=where, device_id_type=MESH,
    )


def kernel(
    sections, groups,
    features, ages, age_table, returns, owners, slots, gain, w_gate, w_up, w_down,
    final_gain, head, old,
    rewards_out, weights_out,
    wg, wu, wd, w_both, state, gathered, hidden, part, part_in, line_out, line_in, last_in,
    final_row, reward_cols, marks, marks_wide, result, prio_wide, tops, shares, spare, sums,
    w_sem,
    in_send, ag_send, ag_recv, rs_send, rs_recv, ln_send, ln_recv, fn_recv,
    mk_send, mk_recv, up_send, up_recv, rw_send, rw_recv, sm_send, sm_recv,
):
    sec = lax.axis_index("section")
    me = lax.axis_index("rows")
    spot = (lax.rem(me, SIDE), me // SIDE)
    block, width = state.shape[2], state.shape[3]
    rows = features.shape[0]
    ff = hidden.shape[1]
    even = ff // 256 * 256
    rest = ff - even
    last = sections - 1
    rounds = MICRO // SIDE

    def step_on(axis, d):
        return lax.rem(spot[axis] + d, SIDE)

    def on_line(axis, index):
        return spot[1] * SIDE + index if axis == 0 else index * SIDE + spot[0]

    loads = [
        pltpu.make_async_copy(w_gate, wg, w_sem.at[0]),
        pltpu.make_async_copy(w_up, wu, w_sem.at[1]),
        pltpu.make_async_copy(w_down, wd, w_sem.at[2]),
    ]
    for load in loads:
        load.start()

    barrier = pltpu.get_barrier_semaphore()
    for j in range(1, groups):
        pl.semaphore_signal(barrier, inc=1, device_id={"rows": lax.rem(me + j, groups)}, device_id_type=MESH)
    for j in range(1, sections):
        pl.semaphore_signal(barrier, inc=1, device_id={"section": lax.rem(sec + j, sections)}, device_id_type=MESH)
    before = lax.rem(sec + last, sections)
    for axis in range(2):
        for d in range(1, SIDE):
            pl.semaphore_signal(
                barrier, inc=1, device_id={"section": before, "rows": on_line(axis, step_on(axis, d))}, device_id_type=MESH
            )

    marks[me] = (owners[...] * (old.shape[0] * LANES) + slots[...]).astype(jnp.float32)

    for i in range(final_gain.shape[0]):
        final_row[0:1, i * LANES:(i + 1) * LANES] = final_gain[i:i + 1, :]
        final_row[1:2, i * LANES:(i + 1) * LANES] = head[i:i + 1, :]

    @pl.when(sec == 0)
    def _():
        tall = jnp.transpose(jnp.broadcast_to(ages[...].astype(jnp.float32), (LANES, rows)))
        buckets = age_table.shape[0]
        onehot = (
            tall[:, :buckets] == lax.broadcasted_iota(jnp.int32, (rows, buckets), 1).astype(jnp.float32)
        ).astype(jnp.float32).astype(jnp.bfloat16)
        for at, size in chunks(width, 512):
            entry = features[:, at:at + size].astype(jnp.float32) + jnp.dot(
                onehot, age_table[:, at:at + size], preferred_element_type=jnp.float32
            )
            entry = entry.astype(jnp.bfloat16).reshape(2, rounds, block, size)
            for h in range(2):
                for k in range(rounds):
                    state[k * SIDE + spot[1 - h], h, :, at:at + size] = entry[h, k]

    def turned(load, flat, first):
        load.wait()
        for at in range(0, even, 256):
            w_both[:, first * even + at:first * even + at + 256] = jnp.transpose(flat[at:at + 256, :])
        w_both[:, 2 * even + first * LANES:2 * even + first * LANES + rest] = jnp.transpose(flat[even:ff, :])

    w_both[:, 2 * even:2 * even + 256] = jnp.zeros((width, 256), jnp.bfloat16)
    turned(loads[0], wg, 0)
    turned(loads[1], wu, 1)
    loads[2].wait()

    pl.semaphore_wait(barrier, groups - 1 + sections - 1 + 2 * (SIDE - 1))

    here = {"rows": lax.rem(me + 1, groups)}

    def arrived(ref, recv):
        remote(ref, ref, in_send.at[0], recv, here).wait_recv()

    def departed(ref, send):
        remote(ref, ref, send, ln_recv.at[0, 0], here).wait_send()

    def to_group(ref, send, recv, j):
        return remote(ref.at[me], ref.at[me], send.at[0], recv.at[0], {"rows": lax.rem(me + j, groups)})

    def all_but_one(ref):
        return ref.at[pl.ds(0, groups - 1)]

    def in_copy(k, h, d):
        t = k * SIDE + spot[1 - h]
        ref = state.at[t, h]
        return remote(ref, ref, in_send.at[0], ln_recv.at[t, h], {"rows": on_line(1 - h, step_on(1 - h, d))})

    def ag_copy(t, h, d):
        ref = gathered.at[t, h, spot[h]]
        return remote(ref, ref, ag_send.at[0], ag_recv.at[lax.rem(t, RING), h], {"rows": on_line(h, step_on(h, d))})

    def rs_copy(t, h, d):
        return remote(
            part.at[t, h, step_on(h, d)], part_in.at[t, h, d - 1], rs_send.at[0], rs_recv.at[lax.rem(t, RING), h],
            {"rows": on_line(h, step_on(h, d))},
        )

    def line_copy(t, h, d):
        return remote(
            line_out.at[t, h], line_in.at[t, h, spot[1 - h]], ln_send.at[0], ln_recv.at[t, h],
            {"section": jnp.minimum(sec + 1, last), "rows": on_line(1 - h, step_on(1 - h, d))},
        )

    def home_of(t):
        return lax.rem(t, SIDE)

    def last_copy(t, h):
        home = home_of(t)
        d = lax.rem(home + SIDE - spot[1 - h] + SIDE - 1, SIDE)
        k = t // SIDE
        return remote(
            line_out.at[t, h], last_in.at[k, h, d], ln_send.at[0], fn_recv.at[k, h],
            {"rows": on_line(1 - h, home)},
        )

    def normed(t, h):
        wide = state[t, h].astype(jnp.float32)
        scale = lax.rsqrt(jnp.mean(wide * wide, axis=-1, keepdims=True) + 1e-06)
        gathered[t, h, spot[h]] = (wide * scale * gain[...]).astype(jnp.bfloat16)

    def enter(t):
        for h in range(2):
            @pl.when(sec > 0)
            def _():
                arrived(line_in.at[t, h], ln_recv.at[t, h])
                total = line_in[t, h, 0].astype(jnp.float32)
                for i in range(1, SIDE):
                    total = total + line_in[t, h, i].astype(jnp.float32)
                state[t, h] = total.astype(jnp.bfloat16)

            @pl.when((sec == 0) & (spot[1 - h] != home_of(t)))
            def _():
                arrived(state.at[t, h], ln_recv.at[t, h])

            normed(t, h)
            for d in (2, 1, 3):
                ag_copy(t, h, d).start()

    def work(t):
        for h in range(2):
            foreign = (sec == 0) & (t == 0) & (spot[1 - h] > 0)

            @pl.when(foreign)
            def _():
                arrived(gathered.at[t, h], ag_recv.at[0, h])

            @pl.when(jnp.logical_not(foreign))
            def _():
                arrived(gathered.at[t, h, pl.ds(0, SIDE - 1)], ag_recv.at[lax.rem(t, RING), h])
        piece = gathered[t].reshape(2 * SIDE * block, width)
        for at in range(0, even, 256):
            gate = jnp.dot(piece, w_both[:, at:at + 256], preferred_element_type=jnp.float32)
            upper = jnp.dot(piece, w_both[:, even + at:even + at + 256], preferred_element_type=jnp.float32)
            hidden[:, at:at + 256] = (gate / (1.0 + jnp.exp(-gate)) * upper).astype(jnp.bfloat16)
        ends = jnp.dot(piece, w_both[:, 2 * even:2 * even + 256], preferred_element_type=jnp.float32)
        gate, upper = ends[:, :rest], ends[:, LANES:LANES + rest]
        hidden[:, even:ff] = (gate / (1.0 + jnp.exp(-gate)) * upper).astype(jnp.bfloat16)
        units = hidden[...]
        for at, size in chunks(width, 256):
            down = jnp.dot(units, wd[:, at:at + size], preferred_element_type=jnp.float32)
            part[t, :, :, :, at:at + size] = down.astype(jnp.bfloat16).reshape(2, SIDE, block, size)
        for d in (2, 1, 3):
            for h in range(2):
                rs_copy(t, h, d).start()

    def leave(t):
        home = home_of(t)
        for h in range(2):
            total = part[t, h, spot[h]].astype(jnp.float32)
            total = total + jnp.where(spot[1 - h] == home, state[t, h].astype(jnp.float32), 0.0)
            arrived(part_in.at[t, h], rs_recv.at[lax.rem(t, RING), h])
            for d in range(1, SIDE):
                total = total + part_in[t, h, d - 1].astype(jnp.float32)
            line_out[t, h] = total.astype(jnp.bfloat16)

            @pl.when(sec < last)
            def _():
                for d in (0, 2, 1, 3):
                    line_copy(t, h, d).start()

            @pl.when((sec == last) & (spot[1 - h] != home))
            def _():
                last_copy(t, h).start()

    def finish(t):
        k = t // SIDE
        for h in range(2):
            @pl.when(spot[1 - h] == home_of(t))
            def _():
                total = line_out[t, h].astype(jnp.float32)
                arrived(last_in.at[k, h], fn_recv.at[k, h])
                for d in range(1, SIDE):
                    total = total + last_in[k, h, d - 1].astype(jnp.float32)
                wide = total.astype(jnp.bfloat16).astype(jnp.float32)
                scale = lax.rsqrt(jnp.mean(wide * wide, axis=-1, keepdims=True) + 1e-06)
                value = jnp.sum(wide * scale * final_row[0:1] * final_row[1:2], axis=-1, keepdims=True)
                reward_cols[h, k] = jnp.broadcast_to(value, (block, LANES))

    @pl.when(sec == 0)
    def _():
        for h in range(2):
            @pl.when(spot[1 - h] == 0)
            def _():
                normed(0, h)
                ref = gathered.at[0, h, spot[h]]
                for j in range(1, groups):
                    remote(ref, ref, ag_send.at[0], ag_recv.at[0, h], {"rows": lax.rem(me + j, groups)}).start()
        for k in range(rounds):
            for h in range(2):
                @pl.when((spot[1 - h] > 0) | (k > 0))
                def _():
                    for d in (2, 1, 3):
                        in_copy(k, h, d).start()

    for j in range(1, groups):
        to_group(marks, mk_send, mk_recv, j).start()

    lines = old.shape[0]
    table = lines * LANES
    tall = lines // sections
    batch = 4
    lane = lax.broadcasted_iota(jnp.int32, (1, LANES), 1).astype(jnp.float32)

    def over_rows(names, join):
        def one(r, best):
            best = list(best)
            for i in range(0, rows, 8):
                mark = marks_wide[r, i:i + 8, :]
                value = prio_wide[r, i:i + 8, :]
                for q in range(batch):
                    best[q] = join(best[q], jnp.where(mark == names[q], value, 0.0))
            return tuple(best)

        return lax.fori_loop(0, groups, one, tuple(jnp.zeros((8, LANES), jnp.float32) for _ in range(batch)))

    soon = [r for r in range(groups) if max(r % SIDE, r // SIDE) < SIDE - 1]
    late = [r for r in range(groups) if r not in soon]
    own_late = (spot[0] == SIDE - 1) | (spot[1] == SIDE - 1)

    def largest(homes, fresh):
        for r in homes:
            prio_wide[r] = jnp.transpose(jnp.broadcast_to(result[r, 1:2], (LANES, rows)))

        def by_name(g, carry):
            names = [marks[g * batch + q] for q in range(batch)]
            best = [jnp.zeros((8, LANES), jnp.float32) if fresh else tops[g * batch + q] for q in range(batch)]
            for r in homes:
                for i in range(0, rows, 8):
                    mark = marks_wide[r, i:i + 8, :]
                    value = prio_wide[r, i:i + 8, :]
                    for q in range(batch):
                        best[q] = jnp.maximum(best[q], jnp.where(mark == names[q], value, 0.0))
            for q in range(batch):
                tops[g * batch + q] = best[q]
            return carry

        lax.fori_loop(0, (groups + tall) // batch, by_name, 0)

    def count():
        arrived(all_but_one(marks), mk_recv.at[0])
        for q in range(tall):
            marks[groups + q] = (me * table + (sec * tall + q) * LANES).astype(jnp.float32) + lane
        for r in range(groups):
            marks_wide[r] = jnp.transpose(jnp.broadcast_to(marks[r], (LANES, rows)))
            prio_wide[r] = jnp.ones((rows, LANES), jnp.float32)

        def by_row(g, carry):
            found = over_rows([marks[g * batch + q] for q in range(batch)], jnp.add)
            for q in range(batch):
                shares[g * batch + q] = 1.0 / jnp.sum(found[q], axis=0, keepdims=True)
            return carry

        lax.fori_loop(0, groups // batch, by_row, 0)

        def by_entry(g, carry):
            first = (me * table + g * (batch * LANES)).astype(jnp.float32)
            found = over_rows([first + (q * LANES) + lane for q in range(batch)], jnp.add)
            for q in range(batch):
                at = pl.ds(g * batch + q, 1)
                spare[at, :] = jnp.where(jnp.sum(found[q], axis=0, keepdims=True) > 0.0, 0.0, old[at, :])
            return carry

        lax.fori_loop(0, lines // batch, by_entry, 0)
        subtotal = jnp.sum(jnp.sum(spare[...], axis=0, keepdims=True), axis=1, keepdims=True)
        sums[me] = jnp.broadcast_to(subtotal, (1, LANES))
        for j in range(1, groups):
            to_group(sums, sm_send, sm_recv, j).start()

    @pl.when(sec >= sections // 2)
    def _():
        count()

    def step(i, carry):
        t = i - ENTER_AHEAD

        @pl.when((sec == last) & (t >= 2))
        def _():
            finish(t - 2)

        @pl.when(t >= 0)
        def _():
            leave(t)

        @pl.when((i + head_start < MICRO) & ((sec > 0) | (i + head_start > 0)))
        def _():
            enter(i + head_start)

        @pl.when((t + WORK_AHEAD >= 0) & (t + WORK_AHEAD < MICRO))
        def _():
            work(t + WORK_AHEAD)

        return carry

    head_start = jnp.where(sec == 0, 1, 0)

    lax.fori_loop(0, MICRO + ENTER_AHEAD, step, 0)

    @pl.when(sec < sections // 2)
    def _():
        count()

    def up_copy(j):
        return remote(result.at[me], result.at[me], up_send.at[0], up_recv.at[0], {"section": last - j})

    @pl.when(sec == last)
    def _():
        finish(MICRO - 2)
        finish(MICRO - 1)
        square = reward_cols[...].reshape(rows, LANES)
        on_diagonal = lax.broadcasted_iota(jnp.int32, (rows, rows), 0) == lax.broadcasted_iota(jnp.int32, (rows, rows), 1)
        row = jnp.sum(jnp.where(on_diagonal, square, 0.0), axis=0, keepdims=True)
        priority = jnp.exp(0.6 * jnp.log(jnp.abs(row - returns[...]) + 0.05))
        result[me, 0:1] = row
        result[me, 1:2] = priority
        for j in range(1, sections):
            up_copy(j).start()


    @pl.when(sec > 0)
    def _():
        departed(part_in, ag_send.at[0])

    departed(part_in, rs_send.at[0])
    departed(all_but_one(marks), mk_send.at[0])

    @pl.when(sec == 0)
    def _():
        departed(part_in.at[pl.ds(0, MICRO - 1)], ag_send.at[0])
        departed(part_in.at[pl.ds(0, rounds - 1)], in_send.at[0])
        for h in range(2):
            @pl.when(spot[1 - h] == 0)
            def _():
                departed(part_in.at[pl.ds(0, 5), 0], ag_send.at[0])

            @pl.when(spot[1 - h] > 0)
            def _():
                departed(part_in.at[0, 0], in_send.at[0])

    arrived(all_but_one(sums), sm_recv.at[0])
    departed(all_but_one(sums), sm_send.at[0])
    kept = sums[0]
    for r in range(1, groups):
        kept = kept + sums[r]

    @pl.when(sec < last)
    def _():
        departed(line_in, ln_send.at[0])
        arrived(result.at[me], up_recv.at[0])

    def give(kind):
        for j in range(1, groups):
            remote(
                result.at[me], result.at[me], rw_send.at[0], rw_recv.at[kind], {"rows": lax.rem(me + j, groups)}
            ).start()

    def take(kind, amount):
        arrived(result.at[pl.ds(0, amount)], rw_recv.at[kind])

    @pl.when(own_late)
    def _():
        give(1)

    @pl.when(jnp.logical_not(own_late))
    def _():
        give(0)

    @pl.when(sec == last)
    def _():
        departed(part_in.at[pl.ds(0, rounds)], ln_send.at[0])

    mine = result[me, 0:1]
    share = rows // sections
    picked = mine[:, 0:share]
    for s in range(1, sections):
        picked = jnp.where(sec == s, mine[:, s * share:(s + 1) * share], picked)
    rewards_out[...] = picked

    @pl.when(own_late)
    def _():
        take(0, len(soon))

    @pl.when(jnp.logical_not(own_late))
    def _():
        take(0, len(soon) - 1)

    largest(soon, True)

    @pl.when(own_late)
    def _():
        take(1, len(late) - 1)

    @pl.when(jnp.logical_not(own_late))
    def _():
        take(1, len(late))

    largest(late, False)
    named = jnp.zeros((1, LANES), jnp.float32)
    for r in range(groups):
        named = named + jnp.max(tops[r], axis=0, keepdims=True) * shares[r]
    scale = table * groups / (kept + jnp.sum(named, axis=1, keepdims=True))
    for q in range(tall):
        top = jnp.max(tops[groups + q], axis=0, keepdims=True)
        weights_out[q:q + 1, :] = jnp.where(top > 0.0, top, old[pl.ds(sec * tall + q, 1), :]) * scale

    departed(all_but_one(result), rw_send.at[0])

    @pl.when(sec == last)
    def _():
        departed(result.at[pl.ds(0, sections - 1)], up_send.at[0])


def handed(rewards, weights, rewards_out, weights_out):
    rewards_out[...] = rewards[...]
    weights_out[...] = weights[...]


def on_device(
    features, ages, age_table, returns, owners, slots, norm_gain,
    w_gate, w_up, w_down, final_gain, reward_head, old_priority,
):
    sections, groups = lax.axis_size("section"), lax.axis_size("rows")
    rows, width = features.shape
    block = rows * groups // (MICRO * 2 * SIDE)
    rounds = MICRO // SIDE
    ff = w_gate.shape[2]
    even = ff // 256 * 256
    table = old_priority.shape[0]
    lines = table // LANES
    vmem = pl.BlockSpec(memory_space=pltpu.VMEM)
    far = pl.BlockSpec(memory_space=pl.ANY)
    bf16, f32, dma = jnp.bfloat16, jnp.float32, pltpu.SemaphoreType.DMA
    rewards, weights = pl.pallas_call(
        functools.partial(kernel, sections, groups),
        out_shape=(
            jax.ShapeDtypeStruct((1, rows // sections), f32),
            jax.ShapeDtypeStruct((lines // sections, LANES), f32),
        ),
        in_specs=[vmem] * 7 + [far] * 3 + [vmem] * 3,
        out_specs=(vmem, vmem),
        scratch_shapes=[
            pltpu.VMEM((ff, width), bf16),
            pltpu.VMEM((ff, width), bf16),
            pltpu.VMEM((ff, width), bf16),
            pltpu.VMEM((width, 2 * even + 256), bf16),
            pltpu.VMEM((MICRO, 2, block, width), bf16),
            pltpu.VMEM((MICRO, 2, SIDE, block, width), bf16),
            pltpu.VMEM((2 * SIDE * block, ff), bf16),
            pltpu.VMEM((MICRO, 2, SIDE, block, width), bf16),
            pltpu.VMEM((MICRO, 2, SIDE - 1, block, width), bf16),
            pltpu.VMEM((MICRO, 2, block, width), bf16),
            pltpu.VMEM((MICRO, 2, SIDE, block, width), bf16),
            pltpu.VMEM((rounds, 2, SIDE - 1, block, width), bf16),
            pltpu.VMEM((2, width), f32),
            pltpu.VMEM((2, rounds, block, LANES), f32),
            pltpu.VMEM((groups + lines // sections, 1, rows), f32),
            pltpu.VMEM((groups, rows, LANES), f32),
            pltpu.VMEM((groups, 2, rows), f32),
            pltpu.VMEM((groups, rows, LANES), f32),
            pltpu.VMEM((groups + lines // sections, 8, LANES), f32),
            pltpu.VMEM((groups, 1, LANES), f32),
            pltpu.VMEM((lines, LANES), f32),
            pltpu.VMEM((groups, 1, LANES), f32),
            dma((3,)),
            dma((1,)),
            dma((1,)), dma((RING, 2)),
            dma((1,)), dma((RING, 2)),
            dma((1,)), dma((MICRO, 2)),
            dma((rounds, 2)),
            dma((1,)), dma((1,)),
            dma((1,)), dma((1,)),
            dma((1,)), dma((2,)),
            dma((1,)), dma((1,)),
        ],
        compiler_params=pltpu.CompilerParams(
            collective_id=0, has_side_effects=True, vmem_limit_bytes=56 * 1024 * 1024
        ),
        name="refresh",
    )(
        features, ages.reshape(1, rows), age_table, returns.reshape(1, rows),
        owners.reshape(1, rows), slots.reshape(1, rows),
        norm_gain, w_gate[0].T, w_up[0].T, w_down[0],
        final_gain.reshape(-1, LANES), reward_head.reshape(-1, LANES),
        old_priority.reshape(lines, LANES),
    )
    rewards, weights = pl.pallas_call(
        handed, out_shape=tuple(jax.ShapeDtypeStruct(each.shape, f32) for each in (rewards, weights)),
        in_specs=[vmem, vmem], out_specs=(vmem, vmem), name="handed",
    )(rewards, weights)
    return rewards.reshape(-1), weights.reshape(-1)


def solution(mesh):
    placed = (
        P("rows", None),
        P("rows"),
        P(),
        P("rows"),
        P("rows", None),
        P("rows"),
        P("section", None),
        P("section", None, "rows"),
        P("section", None, "rows"),
        P("section", "rows", None),
        P(),
        P(),
        P("rows"),
    )
    return jax.shard_map(
        on_device,
        mesh=mesh,
        in_specs=placed,
        out_specs=(P(("rows", "section")), P(("rows", "section"))),
        check_vma=False,
    )
```

```python
import functools

import jax
import jax.numpy as jnp
from jax import lax
from jax.experimental import pallas as pl
from jax.experimental.pallas import tpu as pltpu
from jax.sharding import PartitionSpec as P

MICRO = 32
ENTER_AHEAD = 3
WORK_AHEAD = 2
RING = 4
SIDE = 4
MESH = pl.DeviceIdType.MESH
LANES = 128


def chunks(total, size):
    return [(at, min(size, total - at)) for at in range(0, total, size)]


def remote(src, dst, send_sem, recv_sem, where):
    return pltpu.make_async_remote_copy(
        src_ref=src, dst_ref=dst, send_sem=send_sem, recv_sem=recv_sem,
        device_id=where, device_id_type=MESH,
    )


def kernel(
    sections, groups,
    features, ages, age_table, returns, owners, slots, gain, w_gate, w_up, w_down,
    final_gain, head, old,
    rewards_out, weights_out,
    wg, wu, wd, w_both, state, gathered, hidden, part, part_in, line_out, line_in, last_in,
    final_row, reward_cols, marks, marks_wide, result, prio_wide, tops, shares, spare, sums,
    w_sem,
    in_send, ag_send, ag_recv, rs_send, rs_recv, ln_send, ln_recv, fn_recv,
    mk_send, mk_recv, up_send, up_recv, rw_send, rw_recv, sm_send, sm_recv,
):
    sec = lax.axis_index("section")
    me = lax.axis_index("rows")
    spot = (lax.rem(me, SIDE), me // SIDE)
    block, width = state.shape[2], state.shape[3]
    rows = features.shape[0]
    ff = hidden.shape[1]
    even = ff // 256 * 256
    rest = ff - even
    last = sections - 1
    rounds = MICRO // SIDE

    far_first = sorted(range(1, groups), key=lambda j: -min(j % SIDE, SIDE - j % SIDE) - min(j // SIDE, SIDE - j // SIDE))

    def across(j):
        return {"rows": lax.rem(spot[1] + j // SIDE, SIDE) * SIDE + lax.rem(spot[0] + j % SIDE, SIDE)}

    def step_on(axis, d):
        return lax.rem(spot[axis] + d, SIDE)

    def on_line(axis, index):
        return spot[1] * SIDE + index if axis == 0 else index * SIDE + spot[0]

    loads = [
        pltpu.make_async_copy(w_gate, wg, w_sem.at[0]),
        pltpu.make_async_copy(w_up, wu, w_sem.at[1]),
        pltpu.make_async_copy(w_down, wd, w_sem.at[2]),
    ]
    for load in loads:
        load.start()

    barrier = pltpu.get_barrier_semaphore()
    for j in range(1, groups):
        pl.semaphore_signal(barrier, inc=1, device_id={"rows": lax.rem(me + j, groups)}, device_id_type=MESH)
    for j in range(1, sections):
        pl.semaphore_signal(barrier, inc=1, device_id={"section": lax.rem(sec + j, sections)}, device_id_type=MESH)
    before = lax.rem(sec + last, sections)
    for axis in range(2):
        for d in range(1, SIDE):
            pl.semaphore_signal(
                barrier, inc=1, device_id={"section": before, "rows": on_line(axis, step_on(axis, d))}, device_id_type=MESH
            )

    marks[me] = (owners[...] * (old.shape[0] * LANES) + slots[...]).astype(jnp.float32)

    for i in range(final_gain.shape[0]):
        final_row[0:1, i * LANES:(i + 1) * LANES] = final_gain[i:i + 1, :]
        final_row[1:2, i * LANES:(i + 1) * LANES] = head[i:i + 1, :]

    @pl.when(sec == 0)
    def _():
        tall = jnp.transpose(jnp.broadcast_to(ages[...].astype(jnp.float32), (LANES, rows)))
        buckets = age_table.shape[0]
        onehot = (
            tall[:, :buckets] == lax.broadcasted_iota(jnp.int32, (rows, buckets), 1).astype(jnp.float32)
        ).astype(jnp.float32).astype(jnp.bfloat16)
        for at, size in chunks(width, 512):
            entry = features[:, at:at + size].astype(jnp.float32) + jnp.dot(
                onehot, age_table[:, at:at + size], preferred_element_type=jnp.float32
            )
            entry = entry.astype(jnp.bfloat16).reshape(2, rounds, block, size)
            for h in range(2):
                for k in range(rounds):
                    state[k * SIDE + spot[1 - h], h, :, at:at + size] = entry[h, k]

    def turned(load, flat, first):
        load.wait()
        for at in range(0, even, 256):
            w_both[:, first * even + at:first * even + at + 256] = jnp.transpose(flat[at:at + 256, :])
        w_both[:, 2 * even + first * LANES:2 * even + first * LANES + rest] = jnp.transpose(flat[even:ff, :])

    w_both[:, 2 * even:2 * even + 256] = jnp.zeros((width, 256), jnp.bfloat16)
    turned(loads[0], wg, 0)
    turned(loads[1], wu, 1)
    loads[2].wait()

    pl.semaphore_wait(barrier, groups - 1 + sections - 1 + 2 * (SIDE - 1))

    here = {"rows": lax.rem(me + 1, groups)}

    def arrived(ref, recv):
        remote(ref, ref, in_send.at[0], recv, here).wait_recv()

    def departed(ref, send):
        remote(ref, ref, send, ln_recv.at[0, 0], here).wait_send()

    def to_group(ref, send, recv, j):
        return remote(ref.at[me], ref.at[me], send.at[0], recv.at[0], {"rows": lax.rem(me + j, groups)})

    def all_but_one(ref):
        return ref.at[pl.ds(0, groups - 1)]

    def in_copy(k, h, d):
        t = k * SIDE + spot[1 - h]
        ref = state.at[t, h]
        return remote(ref, ref, in_send.at[0], ln_recv.at[t, h], {"rows": on_line(1 - h, step_on(1 - h, d))})

    def ag_copy(t, h, d):
        ref = gathered.at[t, h, spot[h]]
        return remote(ref, ref, ag_send.at[0], ag_recv.at[lax.rem(t, RING), h], {"rows": on_line(h, step_on(h, d))})

    def rs_copy(t, h, d):
        return remote(
            part.at[t, h, step_on(h, d)], part_in.at[t, h, d - 1], rs_send.at[0], rs_recv.at[lax.rem(t, RING), h],
            {"rows": on_line(h, step_on(h, d))},
        )

    def line_copy(t, h, d):
        return remote(
            line_out.at[t, h], line_in.at[t, h, spot[1 - h]], ln_send.at[0], ln_recv.at[t, h],
            {"section": jnp.minimum(sec + 1, last), "rows": on_line(1 - h, step_on(1 - h, d))},
        )

    def home_of(t):
        return lax.rem(t, SIDE)

    def last_copy(t, h):
        home = home_of(t)
        d = lax.rem(home + SIDE - spot[1 - h] + SIDE - 1, SIDE)
        k = t // SIDE
        return remote(
            line_out.at[t, h], last_in.at[k, h, d], ln_send.at[0], fn_recv.at[k, h],
            {"rows": on_line(1 - h, home)},
        )

    def normed(t, h):
        wide = state[t, h].astype(jnp.float32)
        scale = lax.rsqrt(jnp.mean(wide * wide, axis=-1, keepdims=True) + 1e-06)
        gathered[t, h, spot[h]] = (wide * scale * gain[...]).astype(jnp.bfloat16)

    def enter(t):
        for h in range(2):
            @pl.when(sec > 0)
            def _():
                arrived(line_in.at[t, h], ln_recv.at[t, h])
                total = line_in[t, h, 0].astype(jnp.float32)
                for i in range(1, SIDE):
                    total = total + line_in[t, h, i].astype(jnp.float32)
                state[t, h] = total.astype(jnp.bfloat16)

            @pl.when((sec == 0) & (spot[1 - h] != home_of(t)))
            def _():
                arrived(state.at[t, h], ln_recv.at[t, h])

            normed(t, h)
            for d in (2, 1, 3):
                ag_copy(t, h, d).start()

    def work(t):
        for h in range(2):
            foreign = (sec == 0) & (t == 0) & (spot[1 - h] > 0)

            @pl.when(foreign)
            def _():
                arrived(gathered.at[t, h], ag_recv.at[0, h])

            @pl.when(jnp.logical_not(foreign))
            def _():
                arrived(gathered.at[t, h, pl.ds(0, SIDE - 1)], ag_recv.at[lax.rem(t, RING), h])
        piece = gathered[t].reshape(2 * SIDE * block, width)
        for at in range(0, even, 256):
            gate = jnp.dot(piece, w_both[:, at:at + 256], preferred_element_type=jnp.float32)
            upper = jnp.dot(piece, w_both[:, even + at:even + at + 256], preferred_element_type=jnp.float32)
            hidden[:, at:at + 256] = (gate / (1.0 + jnp.exp(-gate)) * upper).astype(jnp.bfloat16)
        ends = jnp.dot(piece, w_both[:, 2 * even:2 * even + 256], preferred_element_type=jnp.float32)
        gate, upper = ends[:, :rest], ends[:, LANES:LANES + rest]
        hidden[:, even:ff] = (gate / (1.0 + jnp.exp(-gate)) * upper).astype(jnp.bfloat16)
        units = hidden[...]
        for at, size in chunks(width, 256):
            down = jnp.dot(units, wd[:, at:at + size], preferred_element_type=jnp.float32)
            part[t, :, :, :, at:at + size] = down.astype(jnp.bfloat16).reshape(2, SIDE, block, size)
        for d in (2, 1, 3):
            for h in range(2):
                rs_copy(t, h, d).start()

    def leave(t):
        home = home_of(t)
        for h in range(2):
            total = part[t, h, spot[h]].astype(jnp.float32)
            total = total + jnp.where(spot[1 - h] == home, state[t, h].astype(jnp.float32), 0.0)
            arrived(part_in.at[t, h], rs_recv.at[lax.rem(t, RING), h])
            for d in range(1, SIDE):
                total = total + part_in[t, h, d - 1].astype(jnp.float32)
            line_out[t, h] = total.astype(jnp.bfloat16)

            @pl.when(sec < last)
            def _():
                for d in (0, 2, 1, 3):
                    line_copy(t, h, d).start()

            @pl.when((sec == last) & (spot[1 - h] != home))
            def _():
                last_copy(t, h).start()

    def finish(t):
        k = t // SIDE
        for h in range(2):
            @pl.when(spot[1 - h] == home_of(t))
            def _():
                total = line_out[t, h].astype(jnp.float32)
                arrived(last_in.at[k, h], fn_recv.at[k, h])
                for d in range(1, SIDE):
                    total = total + last_in[k, h, d - 1].astype(jnp.float32)
                wide = total.astype(jnp.bfloat16).astype(jnp.float32)
                scale = lax.rsqrt(jnp.mean(wide * wide, axis=-1, keepdims=True) + 1e-06)
                value = jnp.sum(wide * scale * final_row[0:1] * final_row[1:2], axis=-1, keepdims=True)
                reward_cols[h, k] = jnp.broadcast_to(value, (block, LANES))

    @pl.when(sec == 0)
    def _():
        for h in range(2):
            @pl.when(spot[1 - h] == 0)
            def _():
                normed(0, h)
                ref = gathered.at[0, h, spot[h]]
                for j in far_first:
                    remote(ref, ref, ag_send.at[0], ag_recv.at[0, h], across(j)).start()
        for k in range(rounds):
            for h in range(2):
                @pl.when((spot[1 - h] > 0) | (k > 0))
                def _():
                    for d in (2, 1, 3):
                        in_copy(k, h, d).start()

    for j in range(1, groups):
        to_group(marks, mk_send, mk_recv, j).start()

    lines = old.shape[0]
    table = lines * LANES
    tall = lines // sections
    batch = 4
    lane = lax.broadcasted_iota(jnp.int32, (1, LANES), 1).astype(jnp.float32)

    def over_rows(names, join):
        def one(r, best):
            best = list(best)
            for i in range(0, rows, 8):
                mark = marks_wide[r, i:i + 8, :]
                value = prio_wide[r, i:i + 8, :]
                for q in range(batch):
                    best[q] = join(best[q], jnp.where(mark == names[q], value, 0.0))
            return tuple(best)

        return lax.fori_loop(0, groups, one, tuple(jnp.zeros((8, LANES), jnp.float32) for _ in range(batch)))

    soon = [r for r in range(groups) if max(r % SIDE, r // SIDE) < SIDE - 1]
    late = [r for r in range(groups) if r not in soon]
    own_late = (spot[0] == SIDE - 1) | (spot[1] == SIDE - 1)

    def largest(homes, fresh):
        for r in homes:
            prio_wide[r] = jnp.transpose(jnp.broadcast_to(result[r, 1:2], (LANES, rows)))

        def by_name(g, carry):
            names = [marks[g * batch + q] for q in range(batch)]
            best = [jnp.zeros((8, LANES), jnp.float32) if fresh else tops[g * batch + q] for q in range(batch)]
            for r in homes:
                for i in range(0, rows, 8):
                    mark = marks_wide[r, i:i + 8, :]
                    value = prio_wide[r, i:i + 8, :]
                    for q in range(batch):
                        best[q] = jnp.maximum(best[q], jnp.where(mark == names[q], value, 0.0))
            for q in range(batch):
                tops[g * batch + q] = best[q]
            return carry

        lax.fori_loop(0, (groups + tall) // batch, by_name, 0)

    def count():
        arrived(all_but_one(marks), mk_recv.at[0])
        for q in range(tall):
            marks[groups + q] = (me * table + (sec * tall + q) * LANES).astype(jnp.float32) + lane
        for r in range(groups):
            marks_wide[r] = jnp.transpose(jnp.broadcast_to(marks[r], (LANES, rows)))
            prio_wide[r] = jnp.ones((rows, LANES), jnp.float32)

        def by_row(g, carry):
            found = over_rows([marks[g * batch + q] for q in range(batch)], jnp.add)
            for q in range(batch):
                shares[g * batch + q] = 1.0 / jnp.sum(found[q], axis=0, keepdims=True)
            return carry

        lax.fori_loop(0, groups // batch, by_row, 0)

        def by_entry(g, carry):
            first = (me * table + g * (batch * LANES)).astype(jnp.float32)
            found = over_rows([first + (q * LANES) + lane for q in range(batch)], jnp.add)
            for q in range(batch):
                at = pl.ds(g * batch + q, 1)
                spare[at, :] = jnp.where(jnp.sum(found[q], axis=0, keepdims=True) > 0.0, 0.0, old[at, :])
            return carry

        lax.fori_loop(0, lines // batch, by_entry, 0)
        subtotal = jnp.sum(jnp.sum(spare[...], axis=0, keepdims=True), axis=1, keepdims=True)
        sums[me] = jnp.broadcast_to(subtotal, (1, LANES))
        for j in range(1, groups):
            to_group(sums, sm_send, sm_recv, j).start()

    @pl.when(sec >= sections // 2)
    def _():
        count()

    def step(i, carry):
        t = i - ENTER_AHEAD

        @pl.when((sec == last) & (t >= 2))
        def _():
            finish(t - 2)

        @pl.when(t >= 0)
        def _():
            leave(t)

        @pl.when((i + head_start < MICRO) & ((sec > 0) | (i + head_start > 0)))
        def _():
            enter(i + head_start)

        @pl.when((t + WORK_AHEAD >= 0) & (t + WORK_AHEAD < MICRO))
        def _():
            work(t + WORK_AHEAD)

        return carry

    head_start = jnp.where(sec == 0, 1, 0)

    lax.fori_loop(0, MICRO + ENTER_AHEAD, step, 0)

    @pl.when(sec < sections // 2)
    def _():
        count()

    def up_copy(j):
        return remote(result.at[me], result.at[me], up_send.at[0], up_recv.at[0], {"section": last - j})

    @pl.when(sec == last)
    def _():
        finish(MICRO - 2)
        finish(MICRO - 1)
        square = reward_cols[...].reshape(rows, LANES)
        on_diagonal = lax.broadcasted_iota(jnp.int32, (rows, rows), 0) == lax.broadcasted_iota(jnp.int32, (rows, rows), 1)
        row = jnp.sum(jnp.where(on_diagonal, square, 0.0), axis=0, keepdims=True)
        priority = jnp.exp(0.6 * jnp.log(jnp.abs(row - returns[...]) + 0.05))
        result[me, 0:1] = row
        result[me, 1:2] = priority
        for j in sorted(range(1, sections), key=lambda j: abs(j - sections // 2)):
            up_copy(j).start()


    @pl.when(sec > 0)
    def _():
        departed(part_in, ag_send.at[0])

    departed(part_in, rs_send.at[0])
    departed(all_but_one(marks), mk_send.at[0])

    @pl.when(sec == 0)
    def _():
        departed(part_in.at[pl.ds(0, MICRO - 1)], ag_send.at[0])
        departed(part_in.at[pl.ds(0, rounds - 1)], in_send.at[0])
        for h in range(2):
            @pl.when(spot[1 - h] == 0)
            def _():
                departed(part_in.at[pl.ds(0, 5), 0], ag_send.at[0])

            @pl.when(spot[1 - h] > 0)
            def _():
                departed(part_in.at[0, 0], in_send.at[0])

    arrived(all_but_one(sums), sm_recv.at[0])
    departed(all_but_one(sums), sm_send.at[0])
    kept = sums[0]
    for r in range(1, groups):
        kept = kept + sums[r]

    @pl.when(sec < last)
    def _():
        departed(line_in, ln_send.at[0])
        arrived(result.at[me], up_recv.at[0])

    def give(kind):
        for j in far_first:
            remote(result.at[me], result.at[me], rw_send.at[0], rw_recv.at[kind], across(j)).start()

    def take(kind, amount):
        arrived(result.at[pl.ds(0, amount)], rw_recv.at[kind])

    @pl.when(own_late)
    def _():
        give(1)

    @pl.when(jnp.logical_not(own_late))
    def _():
        give(0)

    @pl.when(sec == last)
    def _():
        departed(part_in.at[pl.ds(0, rounds)], ln_send.at[0])

    mine = result[me, 0:1]
    share = rows // sections
    picked = mine[:, 0:share]
    for s in range(1, sections):
        picked = jnp.where(sec == s, mine[:, s * share:(s + 1) * share], picked)
    rewards_out[...] = picked

    @pl.when(own_late)
    def _():
        take(0, len(soon))

    @pl.when(jnp.logical_not(own_late))
    def _():
        take(0, len(soon) - 1)

    largest(soon, True)

    @pl.when(own_late)
    def _():
        take(1, len(late) - 1)

    @pl.when(jnp.logical_not(own_late))
    def _():
        take(1, len(late))

    largest(late, False)
    named = jnp.zeros((1, LANES), jnp.float32)
    for r in range(groups):
        named = named + jnp.max(tops[r], axis=0, keepdims=True) * shares[r]
    scale = table * groups / (kept + jnp.sum(named, axis=1, keepdims=True))
    for q in range(tall):
        top = jnp.max(tops[groups + q], axis=0, keepdims=True)
        weights_out[q:q + 1, :] = jnp.where(top > 0.0, top, old[pl.ds(sec * tall + q, 1), :]) * scale

    departed(all_but_one(result), rw_send.at[0])

    @pl.when(sec == last)
    def _():
        departed(result.at[pl.ds(0, sections - 1)], up_send.at[0])


def handed(rewards, weights, rewards_out, weights_out):
    rewards_out[...] = rewards[...]
    weights_out[...] = weights[...]


def on_device(
    features, ages, age_table, returns, owners, slots, norm_gain,
    w_gate, w_up, w_down, final_gain, reward_head, old_priority,
):
    sections, groups = lax.axis_size("section"), lax.axis_size("rows")
    rows, width = features.shape
    block = rows * groups // (MICRO * 2 * SIDE)
    rounds = MICRO // SIDE
    ff = w_gate.shape[2]
    even = ff // 256 * 256
    table = old_priority.shape[0]
    lines = table // LANES
    vmem = pl.BlockSpec(memory_space=pltpu.VMEM)
    far = pl.BlockSpec(memory_space=pl.ANY)
    bf16, f32, dma = jnp.bfloat16, jnp.float32, pltpu.SemaphoreType.DMA
    rewards, weights = pl.pallas_call(
        functools.partial(kernel, sections, groups),
        out_shape=(
            jax.ShapeDtypeStruct((1, rows // sections), f32),
            jax.ShapeDtypeStruct((lines // sections, LANES), f32),
        ),
        in_specs=[vmem] * 7 + [far] * 3 + [vmem] * 3,
        out_specs=(vmem, vmem),
        scratch_shapes=[
            pltpu.VMEM((ff, width), bf16),
            pltpu.VMEM((ff, width), bf16),
            pltpu.VMEM((ff, width), bf16),
            pltpu.VMEM((width, 2 * even + 256), bf16),
            pltpu.VMEM((MICRO, 2, block, width), bf16),
            pltpu.VMEM((MICRO, 2, SIDE, block, width), bf16),
            pltpu.VMEM((2 * SIDE * block, ff), bf16),
            pltpu.VMEM((MICRO, 2, SIDE, block, width), bf16),
            pltpu.VMEM((MICRO, 2, SIDE - 1, block, width), bf16),
            pltpu.VMEM((MICRO, 2, block, width), bf16),
            pltpu.VMEM((MICRO, 2, SIDE, block, width), bf16),
            pltpu.VMEM((rounds, 2, SIDE - 1, block, width), bf16),
            pltpu.VMEM((2, width), f32),
            pltpu.VMEM((2, rounds, block, LANES), f32),
            pltpu.VMEM((groups + lines // sections, 1, rows), f32),
            pltpu.VMEM((groups, rows, LANES), f32),
            pltpu.VMEM((groups, 2, rows), f32),
            pltpu.VMEM((groups, rows, LANES), f32),
            pltpu.VMEM((groups + lines // sections, 8, LANES), f32),
            pltpu.VMEM((groups, 1, LANES), f32),
            pltpu.VMEM((lines, LANES), f32),
            pltpu.VMEM((groups, 1, LANES), f32),
            dma((3,)),
            dma((1,)),
            dma((1,)), dma((RING, 2)),
            dma((1,)), dma((RING, 2)),
            dma((1,)), dma((MICRO, 2)),
            dma((rounds, 2)),
            dma((1,)), dma((1,)),
            dma((1,)), dma((1,)),
            dma((1,)), dma((2,)),
            dma((1,)), dma((1,)),
        ],
        compiler_params=pltpu.CompilerParams(
            collective_id=0, has_side_effects=True, vmem_limit_bytes=56 * 1024 * 1024
        ),
        name="refresh",
    )(
        features, ages.reshape(1, rows), age_table, returns.reshape(1, rows),
        owners.reshape(1, rows), slots.reshape(1, rows),
        norm_gain, w_gate[0].T, w_up[0].T, w_down[0],
        final_gain.reshape(-1, LANES), reward_head.reshape(-1, LANES),
        old_priority.reshape(lines, LANES),
    )
    rewards, weights = pl.pallas_call(
        handed, out_shape=tuple(jax.ShapeDtypeStruct(each.shape, f32) for each in (rewards, weights)),
        in_specs=[vmem, vmem], out_specs=(vmem, vmem), name="handed",
    )(rewards, weights)
    return rewards.reshape(-1), weights.reshape(-1)


def solution(mesh):
    placed = (
        P("rows", None),
        P("rows"),
        P(),
        P("rows"),
        P("rows", None),
        P("rows"),
        P("section", None),
        P("section", None, "rows"),
        P("section", None, "rows"),
        P("section", "rows", None),
        P(),
        P(),
        P("rows"),
    )
    return jax.shard_map(
        on_device,
        mesh=mesh,
        in_specs=placed,
        out_specs=(P(("rows", "section")), P(("rows", "section"))),
        check_vma=False,
    )
```
